32 devices in a mesh: py: 4 (over y, core), pz: 8 (over z, x).
Axes of the slice: x: 2, y: 2, z: 4, core: 2. Of those that a mesh axis runs over, the one named last changes fastest.
Arguments:
- wavefunctions: float32 [2, 8, 128, 128, 128], P(None, None, 'pz', 'py'), may hold values from -6 to 6
- potential: float32 [128, 128, 128], P('pz', 'py'), may hold values from -4 to 4
- cutoff_sq: int32 [1], replicated, may hold values from 2304 to 4096
- locked_mask: int32 [8], replicated, may hold values 0 or 1
Outputs:
- applied: float32 [2, 8, 128, 128, 128], P(None, None, 'pz', 'py')
- rayleigh: float32 [8], replicated
- residual_norm: float32 [8], replicated
The draws below stay inside these ranges and needn't reach their ends.
All inputs are finite; a program needn't handle non-finite values.
Results may differ from the reference program's by a relative error of at most 0.00005.
Values sent between devices are 32-bit elements; how exact they have to be, the bound alone decides.
A program may use at most 64 MiB of HBM per device.

```python
import math
import jax
import jax.numpy as jnp
from jax import lax

GRID = 128
NB = 8


def place_ends(entries, own_key, least, largest):
    extent = entries.shape
    place = [jax.random.randint(jax.random.fold_in(own_key, axis), (), 0, extent[axis]) for axis in range(len(extent))]
    entries = entries.at[tuple(place)].set(least)
    longest = extent.index(max(extent))
    place[longest] = (place[longest] + 1) % extent[longest]
    return entries.at[tuple(place)].set(largest)


def steps_of(stream_key, dims, pieces, smallest, top_value):
    def one(dim, parts):
        draws = jax.random.uniform(jax.random.fold_in(jax.random.fold_in(stream_key, 6), dim), (parts,), jnp.float32, smallest / len(pieces), top_value / len(pieces))
        return jnp.repeat(jnp.exp(draws), dims[dim] // parts).reshape((-1,) + (1,) * (len(dims) - dim - 1))

    level = one(*pieces[0])
    for cut in pieces[1:]:
        level = level * one(*cut)
    return level


def centred(rng, extent, scale, limit, shards=(), held_as=jnp.bfloat16):
    result = jax.random.normal(rng, extent, jnp.float32) * scale
    if len(shards) > 0:
        result = steps_of(rng, extent, shards, -0.22, 0.18) * result
    return jnp.clip(result, min=-limit, max=limit).astype(held_as)


def setup_inputs(seed: int = 0) -> dict:
    keys = jax.random.split(jax.random.key(seed), 5)
    return {
        "wavefunctions": centred(keys[0], (2, NB, GRID, GRID, GRID), 1.0, 6.0, ((2, 8), (3, 4)), jnp.float32),
        "potential": centred(keys[1], (GRID, GRID, GRID), 1.0, 4.0, ((0, 8), (1, 4)), jnp.float32),
        "cutoff_sq": jax.random.randint(keys[2], (1,), GRID * GRID * 9 // 64, GRID * GRID // 4 + 1).astype(jnp.int32),
        "locked_mask": place_ends((jax.random.randint(keys[3], (NB,), 0, 4) < 1).astype(jnp.int32), jax.random.fold_in(keys[3], 1), 0, 1),
    }


def reference(wavefunctions, potential, cutoff_sq, locked_mask):
    freq = jnp.arange(GRID, dtype=jnp.int32)
    signed = jnp.where(freq < GRID // 2, freq, freq - GRID)
    square = signed * signed
    total = square[:, None, None] + square[None, :, None] + square[None, None, :]
    keep = (total <= cutoff_sq[0]).astype(jnp.float32)
    kinetic = 0.5 * (math.pi / GRID) ** 2 * total.astype(jnp.float32) * keep

    def one_band(pair):
        real_part, imag_part = pair
        field = real_part + 1j * imag_part
        spectrum = jnp.fft.fftn(field)
        back = jnp.fft.ifftn(spectrum * kinetic)
        return (jnp.real(back) + potential * real_part, jnp.imag(back) + potential * imag_part)
    applied_real, applied_imag = lax.map(one_band, (wavefunctions[0], wavefunctions[1]))
    applied = jnp.stack([applied_real, applied_imag])
    norm_sq = lax.optimization_barrier(jnp.sum(wavefunctions * wavefunctions, axis=(0, 2, 3, 4)))
    correlation = lax.optimization_barrier(jnp.sum(wavefunctions * applied, axis=(0, 2, 3, 4)))
    rayleigh = correlation / norm_sq
    residual = applied - rayleigh[None, :, None, None, None] * wavefunctions
    residual_sq = lax.optimization_barrier(jnp.sum(residual * residual, axis=(0, 2, 3, 4)))
    residual_norm = jnp.sqrt(residual_sq / norm_sq) * (1.0 - locked_mask.astype(jnp.float32))
    return (applied, rayleigh, residual_norm)
```

```python
import functools
import math

import jax
import jax.numpy as jnp
import numpy as np
from jax import lax
from jax.experimental import pallas as pl
from jax.experimental.pallas import tpu as pltpu
from jax.sharding import PartitionSpec as P

PREC = lax.Precision.HIGHEST
MESH = pl.DeviceIdType.MESH


def make_tables(length, inverse):
    counter = jnp.arange(length, dtype=jnp.int32)
    phase = counter[:, None] * counter[None, :] % length
    angle = 2.0 * math.pi / length * phase.astype(jnp.float32)
    if inverse:
        return (jnp.cos(angle) / length, jnp.sin(angle) / length)
    return (jnp.cos(angle), -jnp.sin(angle))


def transform(form, pair, tables):
    re, im = pair
    cosines, sines = tables

    def dot(field, table):
        return jnp.einsum(form, field, table, precision=PREC)

    return (dot(re, cosines) - dot(im, sines), dot(re, sines) + dot(im, cosines))


def exchange(pair, axis, split, concat):
    return tuple(
        lax.all_to_all(part, axis, split_axis=split, concat_axis=concat, tiled=True)
        for part in pair
    )


def signed_square(counter, length):
    signed = jnp.where(counter < length // 2, counter, counter - length)
    return signed * signed


def right_matrix(tables):
    cosines, sines = tables
    top = jnp.concatenate([cosines, sines], axis=1)
    return jnp.concatenate([top, jnp.concatenate([-sines, cosines], axis=1)], axis=0)


def fold_rows(length, lanes_of, extra):
    half = length // 2
    group = lanes_of
    reach = {f: math.isqrt(half * half - f * f) for f in range(-half, half)}
    pairs = group // 2
    first_guest = half - extra // 2
    guests = [list(range(first_guest + i, first_guest + i + pairs)) for i in range(0, extra // 2, pairs)]
    hosts = []
    top = first_guest
    while top - pairs > 0 and length - 1 - 2 * reach[top - 1] > 2 and len(hosts) < 8:
        hosts.append(list(range(top - 1, top - 1 - pairs, -1)))
        top -= pairs
    taken = {f for rows in guests + hosts for f in rows}
    plain = [f for f in range(-half, half) if abs(f) not in taken]
    if len(plain) % group or not hosts:
        return None
    hosts = hosts[::-1]
    first = len(plain) // group
    lanes = np.arange(length)
    signed = np.where(lanes < half, lanes, lanes - length)

    def rows_of(groups):
        return [x for rows in groups for f in rows for x in (f, -f)]

    kept_rows = plain + rows_of(hosts)
    order = np.array(kept_rows + rows_of(guests))
    square = np.array(kept_rows)[:, None] ** 2 + signed[None, :] ** 2
    keep = np.ones((len(hosts), group, length), np.float32)
    moves = {}
    for q in range(pairs):
        free = {h: length - 1 - 2 * reach[rows[q]] for h, rows in enumerate(hosts)}
        for g, rows in enumerate(guests):
            f = rows[q]
            at, end = -reach[f], reach[f]
            while at <= end:
                need = end - at + 1
                if not free:
                    return None
                fits = [h for h in free if free[h] >= need]
                h = min(fits, key=lambda h: free[h]) if fits else max(free, key=lambda h: free[h])
                count = min(need, free.pop(h))
                start = reach[hosts[h][q]] + 1
                shift = (start - at) % length
                mask = moves.setdefault((h, g, shift), np.zeros((group, length), np.float32))
                cells = np.arange(start, start + count)
                for e in range(2):
                    mask[2 * q + e, cells] = 1.0
                    keep[h, 2 * q + e, cells] = 0.0
                    square[(first + h) * group + 2 * q + e, cells] = (
                        f * f + np.arange(at, at + count) ** 2)
                at += count
    plan = tuple(sorted(moves))
    masks = np.stack([moves[m] for m in plan] + list(keep))
    return order % length, first, plan, masks, square.astype(np.int32)


def split(field):
    high = field.astype(jnp.bfloat16)
    return high, (field - high.astype(jnp.float32)).astype(jnp.bfloat16)


def left_dot(table_ref, field):
    high, low = split(field)
    size = table_ref.shape[1] // 2
    th, tl = table_ref[:, :size], table_ref[:, size:]
    return jnp.dot(
        jnp.concatenate([th, th, tl], axis=1), jnp.concatenate([high, low, high], axis=0),
        preferred_element_type=jnp.float32)


def right_dot(field, table_ref):
    high, low = split(field)
    size = table_ref.shape[0] // 2
    th, tl = table_ref[:size], table_ref[size:]
    return jnp.dot(
        jnp.concatenate([high, low, high], axis=1), jnp.concatenate([th, th, tl], axis=0),
        preferred_element_type=jnp.float32)


def main_kernel(
    size_y, size_z, step, first, plan,
    u_hbm, pot_ref, cut_ref, sq_ref, xf_ref, xi_ref, lf_ref, li_ref, yf_ref, yi_ref, mask_ref,
    out_hbm, stat_ref,
    u, a1, r1, a2, r2, r3, o, sums, own, every,
    s1, q1, s2, q2, s3, q3, s4, q4, iu, io, sg, qg,
):
    me_y, me_z = lax.axis_index("py"), lax.axis_index("pz")
    _, _, slots, rows_z, rows_y, length = u.shape
    chunks = rows_z // step
    units = slots * chunks
    rows_k = sq_ref.shape[1]
    unit = 2 * step * rows_k
    pitch = a2.shape[1] // size_z
    blocks = size_z * chunks
    hosts = rows_k - first
    groups = length // size_z - rows_k
    count = size_y * size_z
    bands = size_y * slots

    def load(s, c):
        zs = pl.ds(c * step, step)
        return pltpu.make_async_copy(u_hbm.at[:, :, s, zs], u.at[:, :, s, zs], iu.at[s, c])

    def save(s, c):
        zs = pl.ds(c * step, step)
        return pltpu.make_async_copy(o.at[:, :, s, zs], out_hbm.at[:, :, s, zs], io.at[s, c])

    barrier = pltpu.get_barrier_semaphore()
    for d in range(1, size_z):
        pl.semaphore_signal(barrier, inc=1, device_id={"pz": (me_z + d) % size_z}, device_id_type=MESH)
    for d in range(1, size_y):
        pl.semaphore_signal(barrier, inc=1, device_id={"py": (me_y + d) % size_y}, device_id_type=MESH)
    for s in range(slots):
        for c in range(chunks):
            load(s, c).start()
    pl.semaphore_wait(barrier, size_y + size_z - 2)

    def copy1(s, c, d):
        to = (me_y + d) % size_y
        return pltpu.make_async_remote_copy(
            src_ref=a1.at[:, to, s, pl.ds(c * step, step)],
            dst_ref=r1.at[:, s, pl.ds(c * step, step), me_y],
            send_sem=s1.at[s, c, d - 1], recv_sem=q1.at[s, c, d - 1],
            device_id={"py": to}, device_id_type=MESH)

    def rows2(m, c):
        return pl.ds(pl.multiple_of(m * pitch + c * unit, 8), unit)

    def rows_r(m, c):
        return pl.ds(pl.multiple_of((m * chunks + c) * unit, 8), unit)

    def copy2(s, c, d):
        to = (me_z + d) % size_z
        return pltpu.make_async_remote_copy(
            src_ref=a2.at[s, rows2(to, c)], dst_ref=r2.at[s, rows_r(me_z, c)],
            send_sem=s2.at[s, c, d - 1], recv_sem=q2.at[s, c, d - 1],
            device_id={"pz": to}, device_id_type=MESH)

    def copy3(s, c, d):
        to = (me_z + d) % size_z
        return pltpu.make_async_remote_copy(
            src_ref=r2.at[s, rows_r(to, c)], dst_ref=r3.at[s, rows2(me_z, c)],
            send_sem=s3.at[s, c, d - 1], recv_sem=q3.at[s, c, d - 1],
            device_id={"pz": to}, device_id_type=MESH)

    def copy4(s, c, d):
        to = (me_y + d) % size_y
        return pltpu.make_async_remote_copy(
            src_ref=r1.at[:, s, pl.ds(c * step, step), to],
            dst_ref=o.at[:, me_y, s, pl.ds(c * step, step)],
            send_sem=s4.at[s, c, d - 1], recv_sem=q4.at[s, c, d - 1],
            device_id={"py": to}, device_id_type=MESH)

    order_z = sorted(range(1, size_z), key=lambda d: -min(d, size_z - d))
    order_y = sorted(range(1, size_y), key=lambda d: -min(d, size_y - d))

    def forward_x(i):
        s, c = i // chunks, i % chunks
        load(s, c).wait()
        zs = pl.ds(c * step, step)
        for d in order_y + [0]:
            to = (me_y + d) % size_y
            rows = jnp.concatenate(
                [u[p, to, s, zs].reshape(step * rows_y, length) for p in range(2)], axis=1)
            done = right_dot(rows, xf_ref)
            for p in range(2):
                part = done[:, p * length : (p + 1) * length].reshape(step, rows_y, length)
                if d == 0:
                    r1[p, s, zs, me_y] = part
                else:
                    a1[p, to, s, zs] = part
            if d > 0:
                copy1(s, c, d).start()

    def forward_y(i):
        s, c = i // chunks, i % chunks
        for d in range(1, size_y):
            copy1(s, c, d).wait_recv()
        for z in range(0, step, 2):
            sides = []
            for e in range(2):
                sides.append(jnp.concatenate(
                    [r1[p, s, c * step + z + e].reshape(length, length) for p in range(2)], axis=0))
            done = left_dot(yf_ref, jnp.concatenate(sides, axis=1))
            for p in range(2):
                for e in range(2):
                    part = done[p * length : (p + 1) * length, e * length : (e + 1) * length]
                    part = [part[g * size_z : (g + 1) * size_z] for g in range(rows_k + groups)]
                    for h in range(hosts):
                        part[first + h] = part[first + h] * mask_ref[len(plan) + h]
                    for t, (h, g, shift) in enumerate(plan):
                        part[first + h] = part[first + h] + pltpu.roll(
                            part[rows_k + g], shift, axis=1) * mask_ref[t]
                    for g in range(rows_k):
                        a2[s, pl.ds(c * unit + g * 2 * step + p * step + z + e, size_z, stride=pitch)] = part[g]
        for d in order_z:
            copy2(s, c, d).start()
        r2[s, rows_r(me_z, c)] = a2[s, rows2(me_z, c)]

    ahead = min(2, units)
    for i in range(ahead):
        forward_x(i)

    def forward_both(i, carry):
        forward_x(i + ahead)
        forward_y(i)
        return carry
    lax.fori_loop(0, units - ahead, forward_both, 0)

    def forward_rest(i, carry):
        forward_y(i)
        return carry
    lax.fori_loop(units - ahead, units, forward_rest, 0)

    kz = lax.broadcasted_iota(jnp.int32, (length, length), 0)
    kz_sq = signed_square(kz, length)

    def z_rows(s, ks):
        def at(k, p, i):
            return pl.ds(k * 2 * step + p * step + i, blocks, stride=unit)
        sides, weights = [], []
        for k in ks:
            sides.append(jnp.concatenate(
                [r2[s, at(k, p, i)] for p in range(2) for i in range(step)], axis=0))
            weights.append(weigh(kz_sq + sq_ref[me_z, pl.ds(k, 1)], cut_ref, length))
        weight = jnp.concatenate(weights, axis=1)
        spectrum = left_dot(lf_ref, jnp.concatenate(sides, axis=1))
        done = left_dot(li_ref, spectrum * jnp.concatenate([weight, weight], axis=0))
        for e, k in enumerate(ks):
            for p in range(2):
                for i in range(step):
                    r2[s, at(k, p, i)] = done[
                        p * length + i * blocks : p * length + (i + 1) * blocks,
                        e * length : (e + 1) * length]

    for s in range(slots):
        def arrive2(c, carry):
            for d in range(1, size_z):
                copy2(s, c, d).wait_recv()
            return carry
        lax.fori_loop(0, chunks, arrive2, 0)

        def both_z(h, carry):
            z_rows(s, (2 * h, 2 * h + 1))
            return carry
        lax.fori_loop(0, rows_k // 2, both_z, 0)
        if rows_k % 2:
            z_rows(s, (rows_k - 1,))

        def leave3(c, carry):
            for d in order_z:
                copy3(s, c, d).start()
            r3[s, rows2(me_z, c)] = r2[s, rows_r(me_z, c)]
            return carry
        lax.fori_loop(0, chunks, leave3, 0)

    def inverse_y(i):
        s, c = i // chunks, i % chunks
        for d in range(1, size_z):
            copy3(s, c, d).wait_recv()
        for z in range(0, step, 2):
            sides = []
            for e in range(2):
                both = []
                for p in range(2):
                    part = [r3[s, pl.ds(c * unit + g * 2 * step + p * step + z + e, size_z, stride=pitch)]
                            for g in range(rows_k)]
                    guests = [None] * groups
                    for t, (h, g, shift) in enumerate(plan):
                        moved = pltpu.roll(part[first + h] * mask_ref[t], length - shift, axis=1)
                        guests[g] = moved if guests[g] is None else guests[g] + moved
                    for h in range(hosts):
                        part[first + h] = part[first + h] * mask_ref[len(plan) + h]
                    both += part + guests
                sides.append(jnp.concatenate(both, axis=0))
            done = left_dot(yi_ref, jnp.concatenate(sides, axis=1))
            for p in range(2):
                for e in range(2):
                    part = done[p * length : (p + 1) * length, e * length : (e + 1) * length]
                    r1[p, s, c * step + z + e] = part.reshape(size_y, rows_y, length)
        for d in order_y:
            copy4(s, c, d).start()
        zs = pl.ds(c * step, step)
        o[:, me_y, s, zs] = r1[:, s, zs, me_y]

    def inverse_x(i):
        s, c = i // chunks, i % chunks
        zs = pl.ds(c * step, step)
        area = step * rows_y
        pot = pot_ref[zs].reshape(area, length)
        for d in range(size_y):
            owner = (me_y + size_y - d) % size_y
            if d > 0:
                copy4(s, c, d).wait_recv()
            rows = jnp.concatenate(
                [o[p, owner, s, zs].reshape(area, length) for p in range(2)], axis=1)
            done = right_dot(rows, xi_ref)
            fields, results = [], []
            for p in range(2):
                field = u[p, owner, s, zs].reshape(area, length)
                part = done[:, p * length : (p + 1) * length] + pot * field
                o[p, owner, s, zs] = part.reshape(step, rows_y, length)
                fields.append(field.reshape(area // 8, 8, length))
                results.append(part.reshape(area // 8, 8, length))

            def total(values):
                return jnp.sum(values[0] + values[1], axis=0)
            norm = total([f * f for f in fields])
            corr = total([f * r for f, r in zip(fields, results)])
            shift = jnp.where(norm > 0.0, corr / jnp.where(norm > 0.0, norm, 1.0), 0.0)
            gaps = [r - shift[None] * f for f, r in zip(fields, results)]
            values = (norm, corr, shift, total([g * g for g in gaps]),
                      total([g * f for g, f in zip(gaps, fields)]))
            for n, value in enumerate(values):
                sums[n, owner, s, c] = value
        save(s, c).start()

    inverse_y(0)

    def inverse_both(i, carry):
        inverse_y(i)
        inverse_x(i - 1)
        return carry
    lax.fori_loop(1, units, inverse_both, 0)
    inverse_x(units - 1)

    norm, corr, shift, rest_sq, rest_dot = (
        sums[n].reshape(bands, chunks * 8, length) for n in range(5))

    def of_band(value):
        return jnp.sum(jnp.sum(value, axis=1), axis=1, keepdims=True)
    norm_own, corr_own = of_band(norm), of_band(corr)
    shift_own = jnp.where(norm_own > 0.0, corr_own / jnp.where(norm_own > 0.0, norm_own, 1.0), 0.0)
    gap = shift - shift_own[:, :, None]
    sq_own = of_band(rest_sq + gap * (2.0 * rest_dot + gap * norm))
    dot_own = of_band(rest_dot + gap * norm)
    line = lax.broadcasted_iota(jnp.int32, (bands, length), 0)
    lane = lax.broadcasted_iota(jnp.int32, (bands, length), 1)
    packed = jnp.zeros((bands, length), jnp.float32)
    for n, value in enumerate((norm_own, corr_own, shift_own, sq_own, dot_own)):
        packed = jnp.where(lane == n * bands + line, value, packed)
    own[...] = jnp.sum(packed, axis=0, keepdims=True)
    me = me_y * size_z + me_z

    def tell(t):
        to = (me + t) % count
        return pltpu.make_async_remote_copy(
            src_ref=own, dst_ref=every.at[me], send_sem=sg.at[t], recv_sem=qg.at[t],
            device_id={"py": to // size_z, "pz": to % size_z}, device_id_type=MESH)

    def tell_start(t, carry):
        tell(t).start()
        return carry
    lax.fori_loop(1, count, tell_start, 0)
    every[me] = own[...]

    def settle(i, carry):
        s, c = i // chunks, i % chunks
        for d in range(1, size_y):
            copy1(s, c, d).wait_send()
            copy4(s, c, d).wait_send()
        for d in range(1, size_z):
            copy2(s, c, d).wait_send()
            copy3(s, c, d).wait_send()
        save(s, c).wait()
        return carry
    lax.fori_loop(0, units, settle, 0)

    def tell_end(t, carry):
        tell(t).wait()
        return carry
    lax.fori_loop(1, count, tell_end, 0)

    table = every[...].reshape(count, length)
    total = jnp.sum(table, axis=0, keepdims=True)

    def kind(value, n):
        return pltpu.roll(value, length - n * bands, axis=1)
    used = lax.broadcasted_iota(jnp.int32, (1, length), 1) < bands
    norm_sq = jnp.where(used, total, 1.0)
    corr_all = kind(jnp.broadcast_to(total, (8, length)), 1)[:1]
    rayleigh = jnp.where(used, corr_all, 0.0) / norm_sq
    gap = kind(table, 2) - rayleigh
    residual = kind(table, 3) + gap * (2.0 * kind(table, 4) + gap * table)
    residual = jnp.maximum(jnp.sum(residual, axis=0, keepdims=True), 0.0)
    residual = jnp.sqrt(jnp.where(used, residual, 0.0) / norm_sq)
    stat_ref[...] = jnp.concatenate(
        [jnp.broadcast_to(rayleigh, (4, length)), jnp.broadcast_to(residual, (4, length))], axis=0)


def two_parts(table):
    table = np.asarray(table, np.float64).astype(np.float32)
    high = table.astype(jnp.bfloat16)
    low = (table - high.astype(np.float32)).astype(jnp.bfloat16)
    return high, low


def exact_matrix(length, inverse):
    counter = np.arange(length)
    angle = 2.0 * math.pi / length * (counter[:, None] * counter[None, :] % length)
    if inverse:
        cosines, sines = np.cos(angle) / length, np.sin(angle) / length
    else:
        cosines, sines = np.cos(angle), -np.sin(angle)
    return np.block([[cosines, sines], [-sines, cosines]])


def fused_hamiltonian(wavefunctions, potential, cutoff_sq, folding, step):
    order, first, plan, masks, square = folding
    _, bands, rows_z, rows_y, length = wavefunctions.shape
    size_y, size_z = lax.axis_size("py"), lax.axis_size("pz")
    slots = bands // size_y
    rows_k = square.shape[0] // size_z
    chunks = rows_z // step
    unit = 2 * step * rows_k
    pitch = chunks * unit + 8
    blocks = size_z * chunks
    count = size_y * size_z
    xf, xi = exact_matrix(length, False), exact_matrix(length, True)
    both_y = np.concatenate([order, order + length])
    order_z = (step * np.arange(blocks)[None, :] + np.arange(step)[:, None]).reshape(-1)
    both_z = np.concatenate([order_z, order_z + length])
    tables = [np.concatenate(two_parts(t), axis=0) for t in (xf, xi)]
    tables += [np.concatenate(two_parts(t), axis=1)
               for t in (xf.T[:, both_z], xi.T[both_z], xf.T[both_y], xi.T[:, both_y])]
    tables = [jnp.asarray(t) for t in tables]
    squares = np.ascontiguousarray(square.reshape(rows_k, size_z, length).swapaxes(0, 1))
    field = wavefunctions.reshape(2, size_y, slots, rows_z, rows_y, length)
    vmem = pl.BlockSpec(memory_space=pltpu.VMEM)
    smem = pl.BlockSpec(memory_space=pltpu.SMEM)
    hbm = pl.BlockSpec(memory_space=pl.ANY)
    near = pltpu.SemaphoreType.DMA((slots, chunks, size_y - 1))
    far = pltpu.SemaphoreType.DMA((slots, chunks, size_z - 1))
    here = pltpu.SemaphoreType.DMA((slots, chunks))
    each = pltpu.SemaphoreType.DMA((count,))
    f32 = jnp.float32
    applied, stats = pl.pallas_call(
        functools.partial(main_kernel, size_y, size_z, step, first, plan),
        out_shape=(jax.ShapeDtypeStruct(field.shape, f32), jax.ShapeDtypeStruct((8, length), f32)),
        in_specs=[hbm, vmem, smem] + [vmem] * 8,
        out_specs=(hbm, vmem),
        scratch_shapes=[
            pltpu.VMEM(field.shape, f32),
            pltpu.VMEM(field.shape, f32),
            pltpu.VMEM((2, slots, rows_z, size_y, rows_y, length), f32),
            pltpu.VMEM((slots, size_z * pitch, length), f32),
            pltpu.VMEM((slots, blocks * unit, length), f32),
            pltpu.VMEM((slots, size_z * pitch, length), f32),
            pltpu.VMEM(field.shape, f32),
            pltpu.VMEM((5, size_y, slots, chunks, 8, length), f32),
            pltpu.VMEM((1, length), f32),
            pltpu.VMEM((count, 1, length), f32),
            near, near, far, far, far, far, near, near, here, here, each, each,
        ],
        compiler_params=pltpu.CompilerParams(
            collective_id=0, has_side_effects=True, vmem_limit_bytes=67043328),
    )(field, potential, cutoff_sq, jnp.asarray(squares), *tables, jnp.asarray(masks))
    return applied.reshape(wavefunctions.shape), stats[0, :bands], stats[4, :bands]


def gather_kernel(size_y, size_z, own_ref, out_ref, send, recv):
    me_y, me_z = lax.axis_index("py"), lax.axis_index("pz")
    me = me_y * size_z + me_z
    count = size_y * size_z
    barrier = pltpu.get_barrier_semaphore()

    def target(t):
        to = (me + t) % count
        return {"py": to // size_z, "pz": to % size_z}

    def greet(t, carry):
        pl.semaphore_signal(barrier, inc=1, device_id=target(t), device_id_type=MESH)
        return carry
    lax.fori_loop(1, count, greet, 0)
    pl.semaphore_wait(barrier, count - 1)

    def copy(t):
        return pltpu.make_async_remote_copy(
            src_ref=own_ref, dst_ref=out_ref.at[me], send_sem=send.at[t], recv_sem=recv.at[t],
            device_id=target(t), device_id_type=MESH)

    def leave(t, carry):
        copy(t).start()
        return carry
    lax.fori_loop(1, count, leave, 0)
    out_ref[me] = own_ref[...]

    def arrive(t, carry):
        copy(t).wait()
        return carry
    lax.fori_loop(1, count, arrive, 0)


def gather_sums(sums):
    size_y, size_z = lax.axis_size("py"), lax.axis_size("pz")
    count = size_y * size_z
    kinds, bands = sums.shape
    if count > 64:
        return lax.all_gather(sums, ("py", "pz"))
    own = jnp.pad(sums, ((0, 8 - kinds), (0, 128 - bands)))
    vmem = pl.BlockSpec(memory_space=pltpu.VMEM)
    every = pl.pallas_call(
        functools.partial(gather_kernel, size_y, size_z),
        out_shape=jax.ShapeDtypeStruct((count, 8, 128), jnp.float32),
        in_specs=[vmem],
        out_specs=vmem,
        scratch_shapes=[pltpu.SemaphoreType.DMA((count,)), pltpu.SemaphoreType.DMA((count,))],
        compiler_params=pltpu.CompilerParams(collective_id=1, has_side_effects=True),
    )(own)
    return every[:, :kinds, :bands]


def weigh(total, cutoff_sq, length):
    keep = (total <= cutoff_sq[0]).astype(jnp.float32)
    return 0.5 * (math.pi / length) ** 2 * total.astype(jnp.float32) * keep


def plain_kinetic(wavefunctions, kinetic, forward, inverse):
    along_x = "bzyn,kn->bzyk"
    along_y = "bznx,kn->bzkx"
    along_z = "bnyx,kn->bkyx"
    pair = (wavefunctions[0], wavefunctions[1])
    pair = transform(along_x, pair, forward)
    pair = exchange(pair, "py", 0, 2)
    pair = transform(along_y, pair, forward)
    pair = exchange(pair, "pz", 2, 1)
    pair = transform(along_z, pair, forward)
    pair = tuple(part * jnp.swapaxes(kinetic, 0, 1)[None] for part in pair)
    pair = transform(along_z, pair, inverse)
    pair = exchange(pair, "pz", 1, 2)
    pair = transform(along_y, pair, inverse)
    pair = exchange(pair, "py", 2, 0)
    pair = transform(along_x, pair, inverse)
    return jnp.stack(pair)


def body(wavefunctions, potential, cutoff_sq, locked_mask):
    _, bands, rows_z, rows_y, length = wavefunctions.shape
    size_y, size_z = lax.axis_size("py"), lax.axis_size("pz")
    step = 4
    unlocked = 1.0 - locked_mask.astype(jnp.float32)
    fits = size_z == 8 and bands == 8 and length % 128 == 0 and bands % size_y == 0
    fits = fits and rows_z % step == 0 and step * rows_y % 8 == 0
    folding = None
    if fits:
        folding = fold_rows(length, size_z, 3 * size_z) or fold_rows(length, size_z, 2 * size_z)
    if folding is not None:
        applied, rayleigh, residual = fused_hamiltonian(
            wavefunctions, potential, cutoff_sq, folding, step)
        return (applied, rayleigh, residual * unlocked)
    forward = make_tables(length, False)
    inverse = make_tables(length, True)
    rows = length // size_z
    full_sq = signed_square(jnp.arange(length, dtype=jnp.int32), length)
    own = lax.axis_index("pz") * rows + jnp.arange(rows, dtype=jnp.int32)
    own_sq = signed_square(own, length)
    total = own_sq[:, None, None] + full_sq[None, :, None] + full_sq[None, None, :]
    kinetic = weigh(total, cutoff_sq, length)
    back = plain_kinetic(wavefunctions, kinetic, forward, inverse)
    applied = back + potential[None, None] * wavefunctions
    norm_own = jnp.sum(wavefunctions * wavefunctions, axis=(0, 2, 3, 4))
    corr_own = jnp.sum(wavefunctions * applied, axis=(0, 2, 3, 4))
    shift = jnp.where(norm_own > 0.0, corr_own / jnp.where(norm_own > 0.0, norm_own, 1.0), 0.0)
    rest = applied - shift[None, :, None, None, None] * wavefunctions
    rest_sq = jnp.sum(rest * rest, axis=(0, 2, 3, 4))
    rest_dot = jnp.sum(rest * wavefunctions, axis=(0, 2, 3, 4))
    sums = jnp.stack([norm_own, corr_own, shift, rest_sq, rest_dot])
    every = gather_sums(sums)
    norm_all, corr_all, shift_all, sq_all, dot_all = (every[:, i] for i in range(5))
    norm_sq = jnp.sum(norm_all, axis=0)
    rayleigh = jnp.sum(corr_all, axis=0) / norm_sq
    gap = shift_all - rayleigh[None]
    residual_sq = jnp.sum(sq_all + 2.0 * gap * dot_all + gap * gap * norm_all, axis=0)
    residual_sq = jnp.maximum(residual_sq, 0.0)
    residual_norm = jnp.sqrt(residual_sq / norm_sq) * unlocked
    return (applied, rayleigh, residual_norm)


def solution(mesh):
    in_specs = (P(None, None, "pz", "py", None), P("pz", "py", None), P(), P())
    out_specs = (P(None, None, "pz", "py", None), P(), P())
    return jax.shard_map(body, mesh=mesh, in_specs=in_specs, out_specs=out_specs, check_vma=False)
```

```python
import functools
import math

import jax
import jax.numpy as jnp
import numpy as np
from jax import lax
from jax.experimental import pallas as pl
from jax.experimental.pallas import tpu as pltpu
from jax.sharding import PartitionSpec as P

PREC = lax.Precision.HIGHEST
MESH = pl.DeviceIdType.MESH


def make_tables(length, inverse):
    counter = jnp.arange(length, dtype=jnp.int32)
    phase = counter[:, None] * counter[None, :] % length
    angle = 2.0 * math.pi / length * phase.astype(jnp.float32)
    if inverse:
        return (jnp.cos(angle) / length, jnp.sin(angle) / length)
    return (jnp.cos(angle), -jnp.sin(angle))


def transform(form, pair, tables):
    re, im = pair
    cosines, sines = tables

    def dot(field, table):
        return jnp.einsum(form, field, table, precision=PREC)

    return (dot(re, cosines) - dot(im, sines), dot(re, sines) + dot(im, cosines))


def exchange(pair, axis, split, concat):
    return tuple(
        lax.all_to_all(part, axis, split_axis=split, concat_axis=concat, tiled=True)
        for part in pair
    )


def signed_square(counter, length):
    signed = jnp.where(counter < length // 2, counter, counter - length)
    return signed * signed


def right_matrix(tables):
    cosines, sines = tables
    top = jnp.concatenate([cosines, sines], axis=1)
    return jnp.concatenate([top, jnp.concatenate([-sines, cosines], axis=1)], axis=0)


WINDOW = 2


def fold_rows(length, lanes_of, extra):
    half = length // 2
    group = lanes_of
    reach = {f: math.isqrt(half * half - f * f) for f in range(-half, half)}
    pairs = group // 2
    first_guest = half - extra // 2
    guests = [list(range(first_guest + i, first_guest + i + pairs)) for i in range(0, extra // 2, pairs)]
    hosts = []
    top = first_guest
    while top - pairs > 0 and length - 1 - 2 * reach[top - 1] > 2 and len(hosts) < 8:
        hosts.append(list(range(top - 1, top - 1 - pairs, -1)))
        top -= pairs
    taken = {f for rows in guests + hosts for f in rows}
    plain = [f for f in range(-half, half) if abs(f) not in taken]
    if len(plain) % group or not hosts:
        return None
    hosts = hosts[::-1]
    first = len(plain) // group
    lanes = np.arange(length)
    signed = np.where(lanes < half, lanes, lanes - length)

    def rows_of(groups):
        return [x for rows in groups for f in rows for x in (f, -f)]

    kept_rows = plain + rows_of(hosts)
    order = np.array(kept_rows + rows_of(guests))
    square = np.array(kept_rows)[:, None] ** 2 + signed[None, :] ** 2
    keep = np.ones((len(hosts), group, length), np.float32)
    moves = {}
    for q in range(pairs):
        free = {h: length - 1 - 2 * reach[rows[q]] for h, rows in enumerate(hosts)}
        for g, rows in enumerate(guests):
            f = rows[q]
            at, end = -reach[f], reach[f]
            while at <= end:
                need = end - at + 1
                if not free:
                    return None
                fits = [h for h in free if free[h] >= need]
                h = min(fits, key=lambda h: free[h]) if fits else max(free, key=lambda h: free[h])
                count = min(need, free.pop(h))
                start = reach[hosts[h][q]] + 1
                shift = (start - at) % length
                mask = moves.setdefault((h, g, shift), np.zeros((group, length), np.float32))
                cells = np.arange(start, start + count)
                for e in range(2):
                    mask[2 * q + e, cells] = 1.0
                    keep[h, 2 * q + e, cells] = 0.0
                    square[(first + h) * group + 2 * q + e, cells] = (
                        f * f + np.arange(at, at + count) ** 2)
                at += count
    plan = tuple(sorted(moves))
    masks = np.stack([moves[m] for m in plan] + list(keep))
    return order % length, first, plan, masks, square.astype(np.int32)


def split(field):
    high = field.astype(jnp.bfloat16)
    return high, (field - high.astype(jnp.float32)).astype(jnp.bfloat16)


def left_dot(table_ref, field):
    high, low = split(field)
    size = table_ref.shape[1] // 2
    th, tl = table_ref[:, :size], table_ref[:, size:]
    return jnp.dot(
        jnp.concatenate([th, th, tl], axis=1), jnp.concatenate([high, low, high], axis=0),
        preferred_element_type=jnp.float32)


def right_dot(field, table_ref):
    high, low = split(field)
    size = table_ref.shape[0] // 2
    th, tl = table_ref[:size], table_ref[size:]
    return jnp.dot(
        jnp.concatenate([high, low, high], axis=1), jnp.concatenate([th, th, tl], axis=0),
        preferred_element_type=jnp.float32)


def await_all(ref, sem):
    pltpu.make_async_copy(ref, ref, sem).wait()


def main_kernel(
    size_y, size_z, step, first, plan, window,
    u_hbm, cut_ref, locked_ref, xf_hbm, yf_hbm, mask_hbm, lf_hbm, li_hbm, sq_hbm, yi_hbm, xi_hbm, pot_hbm,
    o, every,
    u, xf_ref, yf_ref, mask_ref, lf_ref, li_ref, sq_ref, yi_ref, xi_ref, pot_ref,
    a1, r1, a2, r2, r3, sums, own,
    s1, q1, s2, q2, s3, q3, s4, q4, iu, it, sg, qg,
):
    me_y, me_z = lax.axis_index("py"), lax.axis_index("pz")
    _, _, slots, rows_z, rows_y, length = u.shape
    chunks = rows_z // step
    units = slots * chunks
    rows_k = sq_ref.shape[1]
    unit = 2 * step * rows_k
    pitch = a2.shape[1] // size_z
    blocks = size_z * chunks
    hosts = rows_k - first
    groups = length // size_z - rows_k
    count = size_y * size_z
    bands = size_y * slots

    def load(s, c):
        zs = pl.ds(c * step, step)
        return pltpu.make_async_copy(u_hbm.at[:, :, s, zs], u.at[:, :, s, zs], iu.at[s, c])

    barrier = pltpu.get_barrier_semaphore()
    for d in range(1, size_z):
        pl.semaphore_signal(barrier, inc=1, device_id={"pz": (me_z + d) % size_z}, device_id_type=MESH)
    for d in range(1, size_y):
        pl.semaphore_signal(barrier, inc=1, device_id={"py": (me_y + d) % size_y}, device_id_type=MESH)
    pairs = ((xf_hbm, xf_ref), (yf_hbm, yf_ref), (mask_hbm, mask_ref), (lf_hbm, lf_ref), (li_hbm, li_ref),
             (sq_hbm, sq_ref), (yi_hbm, yi_ref), (xi_hbm, xi_ref), (pot_hbm, pot_ref))
    fetches = [pltpu.make_async_copy(src, dst, it.at[n]) for n, (src, dst) in enumerate(pairs)]
    fetches[0].start()
    load(0, 0).start()
    for fetch in fetches[1:]:
        fetch.start()
    for i in range(1, units):
        load(i // chunks, i % chunks).start()

    def copy1(s, c, d):
        to = (me_y + d) % size_y
        return pltpu.make_async_remote_copy(
            src_ref=a1.at[:, to, s, pl.ds(c * step, step)],
            dst_ref=r1.at[:, s, pl.ds(c * step, step), me_y],
            send_sem=s1, recv_sem=q1.at[s, c],
            device_id={"py": to}, device_id_type=MESH)

    def rows2(m, c):
        return pl.ds(pl.multiple_of(m * pitch + c * unit, 8), unit)

    def rows_r(m, c):
        return pl.ds(pl.multiple_of((m * chunks + c) * unit, 8), unit)

    def copy2(s, c, d):
        to = (me_z + d) % size_z
        return pltpu.make_async_remote_copy(
            src_ref=a2.at[s, rows2(to, c)], dst_ref=r2.at[s, rows_r(me_z, c)],
            send_sem=s2, recv_sem=q2.at[s, c],
            device_id={"pz": to}, device_id_type=MESH)

    def copy3(s, c, d):
        to = (me_z + d) % size_z
        return pltpu.make_async_remote_copy(
            src_ref=r2.at[s, rows_r(to, c)], dst_ref=r3.at[s, rows2(me_z, c)],
            send_sem=s3, recv_sem=q3.at[s, c],
            device_id={"pz": to}, device_id_type=MESH)

    def copy4(s, c, d):
        to = (me_y + d) % size_y
        return pltpu.make_async_remote_copy(
            src_ref=r1.at[:, s, pl.ds(c * step, step), to],
            dst_ref=o.at[:, me_y, s, pl.ds(c * step, step)],
            send_sem=s4, recv_sem=q4.at[s, c],
            device_id={"py": to}, device_id_type=MESH)

    order_z = sorted(range(1, size_z), key=lambda d: -min(d, size_z - d))
    order_y = sorted(range(1, size_y), key=lambda d: -min(d, size_y - d))

    def forward_x(i, leave):
        s, c = i // chunks, i % chunks
        load(s, c).wait()
        zs = pl.ds(c * step, step)
        for d in order_y + [0]:
            to = (me_y + d) % size_y
            rows = jnp.concatenate(
                [u[p, to, s, zs].reshape(step * rows_y, length) for p in range(2)], axis=1)
            done = right_dot(rows, xf_ref)
            for p in range(2):
                part = done[:, p * length : (p + 1) * length].reshape(step, rows_y, length)
                if d == 0:
                    r1[p, s, zs, me_y] = part
                else:
                    a1[p, to, s, zs] = part
            if d > 0 and leave:
                copy1(s, c, d).start()

    def forward_y(i):
        s, c = i // chunks, i % chunks
        await_all(a1.at[:, pl.ds(0, size_y - 1), s, pl.ds(c * step, step)], q1.at[s, c])
        for z in range(0, step, 2):
            sides = []
            for e in range(2):
                sides.append(jnp.concatenate(
                    [r1[p, s, c * step + z + e].reshape(length, length) for p in range(2)], axis=0))
            done = left_dot(yf_ref, jnp.concatenate(sides, axis=1))
            for p in range(2):
                for e in range(2):
                    part = done[p * length : (p + 1) * length, e * length : (e + 1) * length]
                    part = [part[g * size_z : (g + 1) * size_z] for g in range(rows_k + groups)]
                    for h in range(hosts):
                        part[first + h] = part[first + h] * mask_ref[len(plan) + h]
                    for t, (h, g, shift) in enumerate(plan):
                        part[first + h] = part[first + h] + pltpu.roll(
                            part[rows_k + g], shift, axis=1) * mask_ref[t]
                    for g in range(rows_k):
                        a2[s, pl.ds(c * unit + g * 2 * step + p * step + z + e, size_z, stride=pitch)] = part[g]
        r2[s, rows_r(me_z, c)] = a2[s, rows2(me_z, c)]

    def leave2(i):
        for d in order_z:
            copy2(i // chunks, i % chunks, d).start()

    def arrive2(i):
        await_all(a2.at[0, pl.ds(0, (size_z - 1) * unit)], q2.at[i // chunks, i % chunks])

    def leave3(i):
        for d in order_z:
            copy3(i // chunks, i % chunks, d).start()

    def arrive3(i):
        await_all(a2.at[0, pl.ds(0, (size_z - 1) * unit)], q3.at[i // chunks, i % chunks])

    kz = lax.broadcasted_iota(jnp.int32, (length, length), 0)
    kz_sq = signed_square(kz, length)

    def z_rows(s, ks):
        def at(k, p, i):
            return pl.ds(k * 2 * step + p * step + i, blocks, stride=unit)
        sides, weights = [], []
        for k in ks:
            sides.append(jnp.concatenate(
                [r2[s, at(k, p, i)] for p in range(2) for i in range(step)], axis=0))
            weights.append(weigh(kz_sq + sq_ref[me_z, pl.ds(k, 1)], cut_ref, length))
        weight = jnp.concatenate(weights, axis=1)
        spectrum = left_dot(lf_ref, jnp.concatenate(sides, axis=1))
        done = left_dot(li_ref, spectrum * jnp.concatenate([weight, weight], axis=0))
        for e, k in enumerate(ks):
            for p in range(2):
                for i in range(step):
                    r2[s, at(k, p, i)] = done[
                        p * length + i * blocks : p * length + (i + 1) * blocks,
                        e * length : (e + 1) * length]

    def both_z(s):
        def two_rows(h, carry):
            z_rows(s, (2 * h, 2 * h + 1))
            return carry
        lax.fori_loop(0, rows_k // 2, two_rows, 0)
        if rows_k % 2:
            z_rows(s, (rows_k - 1,))

        def keep(c, carry):
            r3[s, rows2(me_z, c)] = r2[s, rows_r(me_z, c)]
            return carry
        lax.fori_loop(0, chunks, keep, 0)

    def inverse_y(i):
        s, c = i // chunks, i % chunks
        for z in range(0, step, 2):
            sides = []
            for e in range(2):
                both = []
                for p in range(2):
                    part = [r3[s, pl.ds(c * unit + g * 2 * step + p * step + z + e, size_z, stride=pitch)]
                            for g in range(rows_k)]
                    guests = [None] * groups
                    for t, (h, g, shift) in enumerate(plan):
                        moved = pltpu.roll(part[first + h] * mask_ref[t], length - shift, axis=1)
                        guests[g] = moved if guests[g] is None else guests[g] + moved
                    for h in range(hosts):
                        part[first + h] = part[first + h] * mask_ref[len(plan) + h]
                    both += part + guests
                sides.append(jnp.concatenate(both, axis=0))
            done = left_dot(yi_ref, jnp.concatenate(sides, axis=1))
            for p in range(2):
                for e in range(2):
                    part = done[p * length : (p + 1) * length, e * length : (e + 1) * length]
                    r1[p, s, c * step + z + e] = part.reshape(size_y, rows_y, length)
        for d in order_y:
            copy4(s, c, d).start()
        zs = pl.ds(c * step, step)
        o[:, me_y, s, zs] = r1[:, s, zs, me_y]

    def inverse_x(i):
        s, c = i // chunks, i % chunks
        zs = pl.ds(c * step, step)
        area = step * rows_y
        pot = pot_ref[zs].reshape(area, length)
        await_all(a1.at[:, pl.ds(0, size_y - 1), s, zs], q4.at[s, c])
        for d in range(size_y):
            owner = (me_y + size_y - d) % size_y
            rows = jnp.concatenate(
                [o[p, owner, s, zs].reshape(area, length) for p in range(2)], axis=1)
            done = right_dot(rows, xi_ref)
            fields, results = [], []
            for p in range(2):
                field = u[p, owner, s, zs].reshape(area, length)
                part = done[:, p * length : (p + 1) * length] + pot * field
                o[p, owner, s, zs] = part.reshape(step, rows_y, length)
                fields.append(field.reshape(area // 8, 8, length))
                results.append(part.reshape(area // 8, 8, length))

            def total(values):
                return jnp.sum(values[0] + values[1], axis=0)
            norm = total([f * f for f in fields])
            corr = total([f * r for f, r in zip(fields, results)])
            shift = jnp.where(norm > 0.0, corr / jnp.where(norm > 0.0, norm, 1.0), 0.0)
            gaps = [r - shift[None] * f for f, r in zip(fields, results)]
            values = (norm, corr, shift, total([g * g for g in gaps]),
                      total([g * f for g, f in zip(gaps, fields)]))
            for n, value in enumerate(values):
                sums[n, owner, s, c] = value

    ahead = min(2, units)
    fetches[0].wait()

    def before(i, carry):
        forward_x(i, False)
        return carry
    lax.fori_loop(0, ahead, before, 0)
    pl.semaphore_wait(barrier, size_y + size_z - 2)

    def depart(i, carry):
        for d in order_y:
            copy1(i // chunks, i % chunks, d).start()
        return carry
    lax.fori_loop(0, ahead, depart, 0)
    for fetch in fetches[1:]:
        fetch.wait()

    def outward(i, carry):
        @pl.when(i + ahead < units)
        def _():
            forward_x(i + ahead, True)
        forward_y(i)

        @pl.when(i >= window)
        def _():
            arrive2(i - window)
        leave2(i)

        @pl.when((i >= window) & ((i - window) % chunks == chunks - 1))
        def _():
            both_z((i - window) // chunks)
        return carry
    lax.fori_loop(0, units, outward, 0)

    def homeward(i, carry):
        @pl.when(i < window)
        def _():
            arrive2(units - window + i)

        @pl.when(i >= window)
        def _():
            arrive3(i - window)

        @pl.when(i < units)
        def _():
            leave3(i)

        @pl.when(i == window - 1)
        def _():
            both_z(slots - 1)

        @pl.when(i >= window)
        def _():
            inverse_y(i - window)

        @pl.when(i > window)
        def _():
            inverse_x(i - window - 1)
        return carry
    lax.fori_loop(0, units + window, homeward, 0)
    inverse_x(units - 1)

    norm, corr, shift, rest_sq, rest_dot = (
        sums[n].reshape(bands, chunks * 8, length) for n in range(5))

    def of_band(value):
        return jnp.sum(jnp.sum(value, axis=1), axis=1, keepdims=True)
    norm_own, corr_own = of_band(norm), of_band(corr)
    shift_own = jnp.where(norm_own > 0.0, corr_own / jnp.where(norm_own > 0.0, norm_own, 1.0), 0.0)
    gap = shift - shift_own[:, :, None]
    sq_own = of_band(rest_sq + gap * (2.0 * rest_dot + gap * norm))
    dot_own = of_band(rest_dot + gap * norm)
    line = lax.broadcasted_iota(jnp.int32, (bands, length), 0)
    lane = lax.broadcasted_iota(jnp.int32, (bands, length), 1)
    packed = jnp.zeros((bands, length), jnp.float32)
    for n, value in enumerate((norm_own, corr_own, shift_own, sq_own, dot_own)):
        packed = jnp.where(lane == n * bands + line, value, packed)
    own[...] = jnp.sum(packed, axis=0, keepdims=True)
    me = me_y * size_z + me_z

    def tell(t):
        to = (me + t) % count
        return pltpu.make_async_remote_copy(
            src_ref=own, dst_ref=every.at[me], send_sem=sg, recv_sem=qg,
            device_id={"py": to // size_z, "pz": to % size_z}, device_id_type=MESH)

    def tell_start(t, carry):
        tell(t).start()
        return carry
    lax.fori_loop(1, count, tell_start, 0)
    every[me] = own[...]
    free = jnp.zeros((1, length), jnp.float32)

    for n in range(bands):
        free = jnp.where(lane[:1] == n, 1.0 - locked_ref[n].astype(jnp.float32), free)
    every[count] = free
    for sem in (s1, s4):
        await_all(a1.at[:, pl.ds(0, size_y - 1)], sem)
    for sem in (s2, s3):
        await_all(a2.at[:, pl.ds(0, (size_z - 1) * chunks * unit)], sem)
    for sem in (sg, qg):
        await_all(every.at[pl.ds(0, count - 1)], sem)


def finish_kernel(bands, applied_ref, every_ref, out_hbm, rayleigh_hbm, residual_hbm, ray, res, sems):
    copies = [pltpu.make_async_copy(src, dst, sems.at[n]) for n, (src, dst) in enumerate(
        ((applied_ref, out_hbm), (ray, rayleigh_hbm), (res, residual_hbm)))]
    copies[0].start()
    count, _, length = every_ref.shape
    count = count - 1
    table = every_ref[pl.ds(0, count)].reshape(count, length)
    total = jnp.broadcast_to(jnp.sum(table, axis=0, keepdims=True), (8, length))
    used = lax.broadcasted_iota(jnp.int32, (8, length), 1) < bands

    def kind(value, n):
        return pltpu.roll(value, length - n * bands, axis=1)
    norm_sq = jnp.where(used, total, 1.0)
    rayleigh = jnp.where(used, kind(total, 1), 0.0) / norm_sq
    gap = kind(table, 2) - rayleigh[:1]
    residual = kind(table, 3) + gap * (2.0 * kind(table, 4) + gap * table)
    residual = jnp.maximum(jnp.sum(residual, axis=0, keepdims=True), 0.0)
    residual = jnp.sqrt(jnp.where(used, residual, 0.0) / norm_sq)
    ray[...] = rayleigh[:1, :bands]
    res[...] = (residual[:1] * every_ref[count])[:, :bands]
    for copy in copies[1:]:
        copy.start()
    for copy in copies:
        copy.wait()


def two_parts(table):
    table = np.asarray(table, np.float64).astype(np.float32)
    high = table.astype(jnp.bfloat16)
    low = (table - high.astype(np.float32)).astype(jnp.bfloat16)
    return high, low


def exact_matrix(length, inverse):
    counter = np.arange(length)
    angle = 2.0 * math.pi / length * (counter[:, None] * counter[None, :] % length)
    if inverse:
        cosines, sines = np.cos(angle) / length, np.sin(angle) / length
    else:
        cosines, sines = np.cos(angle), -np.sin(angle)
    return np.block([[cosines, sines], [-sines, cosines]])


def fused_hamiltonian(wavefunctions, potential, cutoff_sq, locked_mask, folding, step):
    order, first, plan, masks, square = folding
    _, bands, rows_z, rows_y, length = wavefunctions.shape
    size_y, size_z = lax.axis_size("py"), lax.axis_size("pz")
    slots = bands // size_y
    rows_k = square.shape[0] // size_z
    chunks = rows_z // step
    unit = 2 * step * rows_k
    pitch = chunks * unit + 8
    blocks = size_z * chunks
    count = size_y * size_z
    xf, xi = exact_matrix(length, False), exact_matrix(length, True)
    both_y = np.concatenate([order, order + length])
    order_z = (step * np.arange(blocks)[None, :] + np.arange(step)[:, None]).reshape(-1)
    both_z = np.concatenate([order_z, order_z + length])
    tables = [np.concatenate(two_parts(t), axis=0) for t in (xf, xi)]
    tables += [np.concatenate(two_parts(t), axis=1)
               for t in (xf.T[:, both_z], xi.T[both_z], xf.T[both_y], xi.T[:, both_y])]
    tables = [jnp.asarray(t) for t in tables]
    squares = np.ascontiguousarray(square.reshape(rows_k, size_z, length).swapaxes(0, 1))
    xf_t, xi_t, lf_t, li_t, yf_t, yi_t = tables
    field = wavefunctions.reshape(2, size_y, slots, rows_z, rows_y, length)
    vmem = pl.BlockSpec(memory_space=pltpu.VMEM)
    smem = pl.BlockSpec(memory_space=pltpu.SMEM)
    anywhere = pl.BlockSpec(memory_space=pl.ANY)
    hbm = pl.BlockSpec(memory_space=pltpu.HBM)
    here = pltpu.SemaphoreType.DMA((slots, chunks))
    once = pltpu.SemaphoreType.DMA
    f32 = jnp.float32
    in_hbm = functools.partial(pltpu.with_memory_space_constraint, memory_space=pltpu.HBM)
    in_vmem = functools.partial(pltpu.with_memory_space_constraint, memory_space=pltpu.VMEM)
    operands = (xf_t, yf_t, jnp.asarray(masks), lf_t, li_t, jnp.asarray(squares), yi_t, xi_t, potential)
    applied, every = pl.pallas_call(
        functools.partial(main_kernel, size_y, size_z, step, first, plan, WINDOW),
        out_shape=(pltpu.VMEM(field.shape, f32), pltpu.VMEM((count + 1, 1, length), f32)),
        in_specs=[hbm, smem, smem] + [hbm] * len(operands),
        out_specs=(vmem, vmem),
        scratch_shapes=[pltpu.VMEM(field.shape, f32)]
        + [pltpu.VMEM(x.shape, x.dtype) for x in operands]
        + [
            pltpu.VMEM(field.shape, f32),
            pltpu.VMEM((2, slots, rows_z, size_y, rows_y, length), f32),
            pltpu.VMEM((slots, size_z * pitch, length), f32),
            pltpu.VMEM((slots, blocks * unit, length), f32),
            pltpu.VMEM((slots, size_z * pitch, length), f32),
            pltpu.VMEM((5, size_y, slots, chunks, 8, length), f32),
            pltpu.VMEM((1, length), f32),
            once, here, once, here, once, here, once, here, here,
            pltpu.SemaphoreType.DMA((len(operands),)), once, once,
        ],
        compiler_params=pltpu.CompilerParams(
            collective_id=0, has_side_effects=True, vmem_limit_bytes=48 * 1024 * 1024),
    )(in_hbm(field), cutoff_sq, locked_mask, *[in_hbm(x) for x in operands])
    out, rayleigh, residual = pl.pallas_call(
        functools.partial(finish_kernel, bands),
        out_shape=(jax.ShapeDtypeStruct(field.shape, f32), jax.ShapeDtypeStruct((1, bands), f32),
                   jax.ShapeDtypeStruct((1, bands), f32)),
        in_specs=[anywhere, vmem],
        out_specs=(hbm, hbm, hbm),
        scratch_shapes=[pltpu.VMEM((1, bands), f32)] * 2 + [pltpu.SemaphoreType.DMA((3,))],
        compiler_params=pltpu.CompilerParams(vmem_limit_bytes=8 * 1024 * 1024),
    )(in_vmem(applied), in_vmem(every))
    return out.reshape(wavefunctions.shape), rayleigh.reshape(bands), residual.reshape(bands)


def gather_kernel(size_y, size_z, own_ref, out_ref, send, recv):
    me_y, me_z = lax.axis_index("py"), lax.axis_index("pz")
    me = me_y * size_z + me_z
    count = size_y * size_z
    barrier = pltpu.get_barrier_semaphore()

    def target(t):
        to = (me + t) % count
        return {"py": to // size_z, "pz": to % size_z}

    def greet(t, carry):
        pl.semaphore_signal(barrier, inc=1, device_id=target(t), device_id_type=MESH)
        return carry
    lax.fori_loop(1, count, greet, 0)
    pl.semaphore_wait(barrier, count - 1)

    def copy(t):
        return pltpu.make_async_remote_copy(
            src_ref=own_ref, dst_ref=out_ref.at[me], send_sem=send.at[t], recv_sem=recv.at[t],
            device_id=target(t), device_id_type=MESH)

    def leave(t, carry):
        copy(t).start()
        return carry
    lax.fori_loop(1, count, leave, 0)
    out_ref[me] = own_ref[...]

    def arrive(t, carry):
        copy(t).wait()
        return carry
    lax.fori_loop(1, count, arrive, 0)


def gather_sums(sums):
    size_y, size_z = lax.axis_size("py"), lax.axis_size("pz")
    count = size_y * size_z
    kinds, bands = sums.shape
    if count > 64:
        return lax.all_gather(sums, ("py", "pz"))
    own = jnp.pad(sums, ((0, 8 - kinds), (0, 128 - bands)))
    vmem = pl.BlockSpec(memory_space=pltpu.VMEM)
    every = pl.pallas_call(
        functools.partial(gather_kernel, size_y, size_z),
        out_shape=jax.ShapeDtypeStruct((count, 8, 128), jnp.float32),
        in_specs=[vmem],
        out_specs=vmem,
        scratch_shapes=[pltpu.SemaphoreType.DMA((count,)), pltpu.SemaphoreType.DMA((count,))],
        compiler_params=pltpu.CompilerParams(collective_id=1, has_side_effects=True),
    )(own)
    return every[:, :kinds, :bands]


def weigh(total, cutoff_sq, length):
    keep = (total <= cutoff_sq[0]).astype(jnp.float32)
    return 0.5 * (math.pi / length) ** 2 * total.astype(jnp.float32) * keep


def plain_kinetic(wavefunctions, kinetic, forward, inverse):
    along_x = "bzyn,kn->bzyk"
    along_y = "bznx,kn->bzkx"
    along_z = "bnyx,kn->bkyx"
    pair = (wavefunctions[0], wavefunctions[1])
    pair = transform(along_x, pair, forward)
    pair = exchange(pair, "py", 0, 2)
    pair = transform(along_y, pair, forward)
    pair = exchange(pair, "pz", 2, 1)
    pair = transform(along_z, pair, forward)
    pair = tuple(part * jnp.swapaxes(kinetic, 0, 1)[None] for part in pair)
    pair = transform(along_z, pair, inverse)
    pair = exchange(pair, "pz", 1, 2)
    pair = transform(along_y, pair, inverse)
    pair = exchange(pair, "py", 2, 0)
    pair = transform(along_x, pair, inverse)
    return jnp.stack(pair)


def body(wavefunctions, potential, cutoff_sq, locked_mask):
    _, bands, rows_z, rows_y, length = wavefunctions.shape
    size_y, size_z = lax.axis_size("py"), lax.axis_size("pz")
    step = 4
    unlocked = 1.0 - locked_mask.astype(jnp.float32)
    fits = size_z == 8 and bands == 8 and length % 128 == 0 and bands % size_y == 0
    fits = fits and rows_z % step == 0 and step * rows_y % 8 == 0
    folding = None
    if fits:
        folding = fold_rows(length, size_z, 3 * size_z) or fold_rows(length, size_z, 2 * size_z)
    if folding is not None:
        return fused_hamiltonian(
            wavefunctions, potential, cutoff_sq, locked_mask, folding, step)
    forward = make_tables(length, False)
    inverse = make_tables(length, True)
    rows = length // size_z
    full_sq = signed_square(jnp.arange(length, dtype=jnp.int32), length)
    own = lax.axis_index("pz") * rows + jnp.arange(rows, dtype=jnp.int32)
    own_sq = signed_square(own, length)
    total = own_sq[:, None, None] + full_sq[None, :, None] + full_sq[None, None, :]
    kinetic = weigh(total, cutoff_sq, length)
    back = plain_kinetic(wavefunctions, kinetic, forward, inverse)
    applied = back + potential[None, None] * wavefunctions
    norm_own = jnp.sum(wavefunctions * wavefunctions, axis=(0, 2, 3, 4))
    corr_own = jnp.sum(wavefunctions * applied, axis=(0, 2, 3, 4))
    shift = jnp.where(norm_own > 0.0, corr_own / jnp.where(norm_own > 0.0, norm_own, 1.0), 0.0)
    rest = applied - shift[None, :, None, None, None] * wavefunctions
    rest_sq = jnp.sum(rest * rest, axis=(0, 2, 3, 4))
    rest_dot = jnp.sum(rest * wavefunctions, axis=(0, 2, 3, 4))
    sums = jnp.stack([norm_own, corr_own, shift, rest_sq, rest_dot])
    every = gather_sums(sums)
    norm_all, corr_all, shift_all, sq_all, dot_all = (every[:, i] for i in range(5))
    norm_sq = jnp.sum(norm_all, axis=0)
    rayleigh = jnp.sum(corr_all, axis=0) / norm_sq
    gap = shift_all - rayleigh[None]
    residual_sq = jnp.sum(sq_all + 2.0 * gap * dot_all + gap * gap * norm_all, axis=0)
    residual_sq = jnp.maximum(residual_sq, 0.0)
    residual_norm = jnp.sqrt(residual_sq / norm_sq) * unlocked
    return (applied, rayleigh, residual_norm)


def solution(mesh):
    in_specs = (P(None, None, "pz", "py", None), P("pz", "py", None), P(), P())
    out_specs = (P(None, None, "pz", "py", None), P(), P())
    return jax.shard_map(body, mesh=mesh, in_specs=in_specs, out_specs=out_specs, check_vma=False)
```

```python
import functools
import math

import jax
import jax.numpy as jnp
import numpy as np
from jax import lax
from jax.experimental import pallas as pl
from jax.experimental.pallas import tpu as pltpu
from jax.sharding import PartitionSpec as P

PREC = lax.Precision.HIGHEST
MESH = pl.DeviceIdType.MESH


def make_tables(length, inverse):
    counter = jnp.arange(length, dtype=jnp.int32)
    phase = counter[:, None] * counter[None, :] % length
    angle = 2.0 * math.pi / length * phase.astype(jnp.float32)
    if inverse:
        return (jnp.cos(angle) / length, jnp.sin(angle) / length)
    return (jnp.cos(angle), -jnp.sin(angle))


def transform(form, pair, tables):
    re, im = pair
    cosines, sines = tables

    def dot(field, table):
        return jnp.einsum(form, field, table, precision=PREC)

    return (dot(re, cosines) - dot(im, sines), dot(re, sines) + dot(im, cosines))


def exchange(pair, axis, split, concat):
    return tuple(
        lax.all_to_all(part, axis, split_axis=split, concat_axis=concat, tiled=True)
        for part in pair
    )


def signed_square(counter, length):
    signed = jnp.where(counter < length // 2, counter, counter - length)
    return signed * signed


def right_matrix(tables):
    cosines, sines = tables
    top = jnp.concatenate([cosines, sines], axis=1)
    return jnp.concatenate([top, jnp.concatenate([-sines, cosines], axis=1)], axis=0)


WINDOW = 2


def fold_rows(length, lanes_of, extra):
    half = length // 2
    group = lanes_of
    reach = {f: math.isqrt(half * half - f * f) for f in range(-half, half)}
    pairs = group // 2
    first_guest = half - extra // 2
    guests = [list(range(first_guest + i, first_guest + i + pairs)) for i in range(0, extra // 2, pairs)]
    hosts = []
    top = first_guest
    while top - pairs > 0 and length - 1 - 2 * reach[top - 1] > 2 and len(hosts) < 8:
        hosts.append(list(range(top - 1, top - 1 - pairs, -1)))
        top -= pairs
    taken = {f for rows in guests + hosts for f in rows}
    plain = [f for f in range(-half, half) if abs(f) not in taken]
    if len(plain) % group or not hosts:
        return None
    hosts = hosts[::-1]
    first = len(plain) // group
    lanes = np.arange(length)
    signed = np.where(lanes < half, lanes, lanes - length)

    def rows_of(groups):
        return [x for rows in groups for f in rows for x in (f, -f)]

    kept_rows = plain + rows_of(hosts)
    order = np.array(kept_rows + rows_of(guests))
    square = np.array(kept_rows)[:, None] ** 2 + signed[None, :] ** 2
    keep = np.ones((len(hosts), group, length), np.float32)
    moves = {}
    for q in range(pairs):
        free = {h: length - 1 - 2 * reach[rows[q]] for h, rows in enumerate(hosts)}
        for g, rows in enumerate(guests):
            f = rows[q]
            at, end = -reach[f], reach[f]
            while at <= end:
                need = end - at + 1
                if not free:
                    return None
                fits = [h for h in free if free[h] >= need]
                h = min(fits, key=lambda h: free[h]) if fits else max(free, key=lambda h: free[h])
                count = min(need, free.pop(h))
                start = reach[hosts[h][q]] + 1
                shift = (start - at) % length
                mask = moves.setdefault((h, g, shift), np.zeros((group, length), np.float32))
                cells = np.arange(start, start + count)
                for e in range(2):
                    mask[2 * q + e, cells] = 1.0
                    keep[h, 2 * q + e, cells] = 0.0
                    square[(first + h) * group + 2 * q + e, cells] = (
                        f * f + np.arange(at, at + count) ** 2)
                at += count
    plan = tuple(sorted(moves))
    masks = np.stack([moves[m] for m in plan] + list(keep))
    return order % length, first, plan, masks, square.astype(np.int32)


def split(field):
    high = field.astype(jnp.bfloat16)
    return high, (field - high.astype(jnp.float32)).astype(jnp.bfloat16)


def left_dot(table_ref, field):
    high, low = split(field)
    size = table_ref.shape[1] // 2
    th, tl = table_ref[:, :size], table_ref[:, size:]
    return jnp.dot(
        jnp.concatenate([th, th, tl], axis=1), jnp.concatenate([high, low, high], axis=0),
        preferred_element_type=jnp.float32)


def right_dot(field, table_ref):
    high, low = split(field)
    size = table_ref.shape[0] // 2
    th, tl = table_ref[:size], table_ref[size:]
    return jnp.dot(
        jnp.concatenate([high, low, high], axis=1), jnp.concatenate([th, th, tl], axis=0),
        preferred_element_type=jnp.float32)


def await_all(ref, sem):
    pltpu.make_async_copy(ref, ref, sem).wait()


def main_kernel(
    size_y, size_z, step, first, plan, window,
    u_hbm, cut_ref, locked_hbm, xf_hbm, yf_hbm, mask_hbm, lf_hbm, li_hbm, sq_hbm, yi_hbm, xi_hbm, pot_hbm,
    o, every,
    u, locked_ref, xf_ref, yf_ref, mask_ref, lf_ref, li_ref, sq_ref, yi_ref, xi_ref, pot_ref,
    a1, r1, a2, r2, r3, sums, own,
    s1, q1, s2, q2, s3, q3, s4, q4, iu, it, sg, qg,
):
    me_y, me_z = lax.axis_index("py"), lax.axis_index("pz")
    _, _, slots, rows_z, rows_y, length = u.shape
    rows_k = sq_ref.shape[1]
    per = rows_z // step + 1
    units = slots * per
    pitch = a2.shape[1] // size_z
    hosts = rows_k - first
    groups = length // size_z - rows_k
    count = size_y * size_z
    bands = size_y * slots

    def is_whole(i):
        return (i >= 2) & (i < units - 2)

    def place(i, whole):
        s, c = i // per, i % per
        big = 2 * step * rows_k
        small = big // 2 + 4
        if whole:
            n = c - 2 * (1 - s)
            return s, step * (1 - s + n), step, 2 * small * (1 - s) + big * n, big
        n = c - (per - 2) * s
        return (s, (per - 2) * step * s + step // 2 * n, step // 2,
                (per - 2) * big * s + small * n, small)

    def each(i, act):
        if isinstance(i, int):
            act(i, 2 <= i < units - 2)
            return

        @pl.when(is_whole(i))
        def _():
            act(i, True)

        @pl.when(jnp.logical_not(is_whole(i)))
        def _():
            act(i, False)

    def load(i, whole):
        s, z, n, _, _ = place(i, whole)
        zs = pl.ds(z, n)
        return pltpu.make_async_copy(u_hbm.at[:, :, s, zs], u.at[:, :, s, zs], iu.at[i])

    barrier = pltpu.get_barrier_semaphore()
    for d in range(1, size_z):
        pl.semaphore_signal(barrier, inc=1, device_id={"pz": (me_z + d) % size_z}, device_id_type=MESH)
    for d in range(1, size_y):
        pl.semaphore_signal(barrier, inc=1, device_id={"py": (me_y + d) % size_y}, device_id_type=MESH)
    pairs = ((locked_hbm, locked_ref), (xf_hbm, xf_ref), (yf_hbm, yf_ref), (mask_hbm, mask_ref), (lf_hbm, lf_ref), (li_hbm, li_ref),
             (sq_hbm, sq_ref), (yi_hbm, yi_ref), (xi_hbm, xi_ref), (pot_hbm, pot_ref))
    fetches = [pltpu.make_async_copy(src, dst, it.at[n]) for n, (src, dst) in enumerate(pairs)]
    fetches[1].start()
    for i in range(2):
        load(i, False).start()
    for n, fetch in enumerate(fetches):
        if n != 1:
            fetch.start()
    for i in range(2, units):
        load(i, 2 <= i < units - 2).start()

    def copy1(i, whole, d):
        s, z, n, _, _ = place(i, whole)
        to = (me_y + d) % size_y
        return pltpu.make_async_remote_copy(
            src_ref=a1.at[:, to, s, pl.ds(z, n)], dst_ref=r1.at[:, s, pl.ds(z, n), me_y],
            send_sem=s1, recv_sem=q1.at[i], device_id={"py": to}, device_id_type=MESH)

    def rows_at(m, base, count):
        return pl.ds(pl.multiple_of(m * pitch + base, 8), count)

    def copy2(i, whole, d):
        s, _, _, base, rows = place(i, whole)
        to = (me_z + d) % size_z
        return pltpu.make_async_remote_copy(
            src_ref=a2.at[s, rows_at(to, base, rows)], dst_ref=r2.at[s, rows_at(me_z, base, rows)],
            send_sem=s2, recv_sem=q2.at[i], device_id={"pz": to}, device_id_type=MESH)

    def copy3(i, whole, d):
        s, _, _, base, rows = place(i, whole)
        to = (me_z + d) % size_z
        return pltpu.make_async_remote_copy(
            src_ref=r2.at[s, rows_at(to, base, rows)], dst_ref=r3.at[s, rows_at(me_z, base, rows)],
            send_sem=s3, recv_sem=q3.at[i], device_id={"pz": to}, device_id_type=MESH)

    def copy4(i, whole, d):
        s, z, n, _, _ = place(i, whole)
        to = (me_y + d) % size_y
        return pltpu.make_async_remote_copy(
            src_ref=r1.at[:, s, pl.ds(z, n), to], dst_ref=o.at[:, me_y, s, pl.ds(z, n)],
            send_sem=s4, recv_sem=q4.at[i], device_id={"py": to}, device_id_type=MESH)

    order_z = sorted(range(1, size_z), key=lambda d: -min(d, size_z - d))
    order_y = sorted(range(1, size_y), key=lambda d: -min(d, size_y - d))

    def forward_x(i, whole, leave=True):
        s, z, n, _, _ = place(i, whole)
        load(i, whole).wait()
        zs = pl.ds(z, n)
        for d in order_y + [0]:
            to = (me_y + d) % size_y
            rows = jnp.concatenate(
                [u[p, to, s, zs].reshape(n * rows_y, length) for p in range(2)], axis=1)
            done = right_dot(rows, xf_ref)
            for p in range(2):
                part = done[:, p * length : (p + 1) * length].reshape(n, rows_y, length)
                if d == 0:
                    r1[p, s, zs, me_y] = part
                else:
                    a1[p, to, s, zs] = part
            if d > 0 and leave:
                copy1(i, whole, d).start()

    def packed(i, whole, g, p, z):
        _, _, n, base, _ = place(i, whole)
        return base + g * 2 * n + p * n + z

    def forward_y(i, whole):
        s, first_z, n, base, count_rows = place(i, whole)
        await_all(a1.at[:, pl.ds(0, size_y - 1), s, pl.ds(first_z, n)], q1.at[i])
        for z in range(0, n, 2):
            sides = []
            for e in range(2):
                sides.append(jnp.concatenate(
                    [r1[p, s, first_z + z + e].reshape(length, length) for p in range(2)], axis=0))
            done = left_dot(yf_ref, jnp.concatenate(sides, axis=1))
            for p in range(2):
                for e in range(2):
                    part = done[p * length : (p + 1) * length, e * length : (e + 1) * length]
                    part = [part[g * size_z : (g + 1) * size_z] for g in range(rows_k + groups)]
                    for h in range(hosts):
                        part[first + h] = part[first + h] * mask_ref[len(plan) + h]
                    for t, (h, g, shift) in enumerate(plan):
                        part[first + h] = part[first + h] + pltpu.roll(
                            part[rows_k + g], shift, axis=1) * mask_ref[t]
                    for g in range(rows_k):
                        a2[s, pl.ds(packed(i, whole, g, p, z + e), size_z, stride=pitch)] = part[g]
        r2[s, rows_at(me_z, base, count_rows)] = a2[s, rows_at(me_z, base, count_rows)]

    def leave2(i, whole):
        for d in order_z:
            copy2(i, whole, d).start()

    def arrive2(i, whole):
        await_all(a2.at[0, pl.ds(0, (size_z - 1) * place(i, whole)[4])], q2.at[i])

    def leave3(i, whole):
        for d in order_z:
            copy3(i, whole, d).start()

    def arrive3(i, whole):
        await_all(a2.at[0, pl.ds(0, (size_z - 1) * place(i, whole)[4])], q3.at[i])

    kz = lax.broadcasted_iota(jnp.int32, (length, length), 0)
    kz_sq = signed_square(kz, length)

    def z_rows(s, ks):
        spots = []
        for i in range(s * per, s * per + per):
            whole = 2 <= i < units - 2
            spots += [(i, whole, z) for z in range(place(i, whole)[2])]

        def at(k, p, spot):
            i, whole, z = spot
            return pl.ds(packed(i, whole, k, p, z), size_z, stride=pitch)
        sides, weights = [], []
        for k in ks:
            sides.append(jnp.concatenate(
                [r2[s, at(k, p, spot)] for p in range(2) for spot in spots], axis=0))
            weights.append(weigh(kz_sq + sq_ref[me_z, pl.ds(k, 1)], cut_ref, length))
        weight = jnp.concatenate(weights, axis=1)
        spectrum = left_dot(lf_ref, jnp.concatenate(sides, axis=1))
        done = left_dot(li_ref, spectrum * jnp.concatenate([weight, weight], axis=0))
        for e, k in enumerate(ks):
            for p in range(2):
                for n, spot in enumerate(spots):
                    top = p * length + n * size_z
                    r2[s, at(k, p, spot)] = done[top : top + size_z, e * length : (e + 1) * length]

    def both_z(s):
        def two_rows(h, carry):
            z_rows(s, (2 * h, 2 * h + 1))
            return carry
        lax.fori_loop(0, rows_k // 2, two_rows, 0)
        if rows_k % 2:
            z_rows(s, (rows_k - 1,))
        r3[s, rows_at(me_z, 0, pitch)] = r2[s, rows_at(me_z, 0, pitch)]

    def inverse_y(i, whole):
        s, first_z, n, _, _ = place(i, whole)
        for z in range(0, n, 2):
            sides = []
            for e in range(2):
                both = []
                for p in range(2):
                    part = [r3[s, pl.ds(packed(i, whole, g, p, z + e), size_z, stride=pitch)]
                            for g in range(rows_k)]
                    guests = [None] * groups
                    for t, (h, g, shift) in enumerate(plan):
                        moved = pltpu.roll(part[first + h] * mask_ref[t], length - shift, axis=1)
                        guests[g] = moved if guests[g] is None else guests[g] + moved
                    for h in range(hosts):
                        part[first + h] = part[first + h] * mask_ref[len(plan) + h]
                    both += part + guests
                sides.append(jnp.concatenate(both, axis=0))
            done = left_dot(yi_ref, jnp.concatenate(sides, axis=1))
            for p in range(2):
                for e in range(2):
                    part = done[p * length : (p + 1) * length, e * length : (e + 1) * length]
                    r1[p, s, first_z + z + e] = part.reshape(size_y, rows_y, length)
        for d in order_y:
            copy4(i, whole, d).start()
        zs = pl.ds(first_z, n)
        o[:, me_y, s, zs] = r1[:, s, zs, me_y]

    def inverse_x(i, whole):
        s, z, n, _, _ = place(i, whole)
        zs = pl.ds(z, n)
        area = n * rows_y
        pot = pot_ref[zs].reshape(area, length)
        await_all(a1.at[:, pl.ds(0, size_y - 1), s, zs], q4.at[i])
        for d in range(size_y):
            owner = (me_y + size_y - d) % size_y
            rows = jnp.concatenate(
                [o[p, owner, s, zs].reshape(area, length) for p in range(2)], axis=1)
            done = right_dot(rows, xi_ref)
            fields, results = [], []
            for p in range(2):
                field = u[p, owner, s, zs].reshape(area, length)
                part = done[:, p * length : (p + 1) * length] + pot * field
                o[p, owner, s, zs] = part.reshape(n, rows_y, length)
                fields.append(field.reshape(area // 8, 8, length))
                results.append(part.reshape(area // 8, 8, length))

            def total(values):
                return jnp.sum(values[0] + values[1], axis=0)
            norm = total([f * f for f in fields])
            corr = total([f * r for f, r in zip(fields, results)])
            shift = jnp.where(norm > 0.0, corr / jnp.where(norm > 0.0, norm, 1.0), 0.0)
            gaps = [r - shift[None] * f for f, r in zip(fields, results)]
            values = (norm, corr, shift, total([g * g for g in gaps]),
                      total([g * f for g, f in zip(gaps, fields)]))
            for k, value in enumerate(values):
                sums[k, owner, s, i % per] = value

    fetches[1].wait()

    def before(i, carry):
        forward_x(i, False, False)
        return carry
    lax.fori_loop(0, 2, before, 0)
    pl.semaphore_wait(barrier, size_y + size_z - 2)
    for i in range(2):
        for d in order_y:
            copy1(i, False, d).start()
    for n, fetch in enumerate(fetches):
        if n != 1:
            fetch.wait()

    def outward(i, carry):
        @pl.when(i + 2 < units)
        def _():
            each(i + 2, forward_x)
        each(i, forward_y)

        @pl.when(i >= window)
        def _():
            each(i - window, arrive2)
        each(i, leave2)

        @pl.when(i == per - 1 + window)
        def _():
            both_z(0)
        return carry
    lax.fori_loop(0, units, outward, 0)

    def homeward(i, carry):
        @pl.when(i < window)
        def _():
            each(units - window + i, arrive2)

        @pl.when(i >= window)
        def _():
            each(i - window, arrive3)

        @pl.when(i < units)
        def _():
            each(i, leave3)

        @pl.when(i == per - 2)
        def _():
            both_z(1)

        @pl.when(i >= window)
        def _():
            each(i - window, inverse_y)

        @pl.when(i > window + 1)
        def _():
            each(i - window - 2, inverse_x)
        return carry
    lax.fori_loop(0, units + window, homeward, 0)
    for i in range(units - 2, units):
        inverse_x(i, False)

    norm, corr, shift, rest_sq, rest_dot = (
        sums[n].reshape(bands, per * 8, length) for n in range(5))

    def of_band(value):
        return jnp.sum(jnp.sum(value, axis=1), axis=1, keepdims=True)
    norm_own, corr_own = of_band(norm), of_band(corr)
    shift_own = jnp.where(norm_own > 0.0, corr_own / jnp.where(norm_own > 0.0, norm_own, 1.0), 0.0)
    gap = shift - shift_own[:, :, None]
    sq_own = of_band(rest_sq + gap * (2.0 * rest_dot + gap * norm))
    dot_own = of_band(rest_dot + gap * norm)
    line = lax.broadcasted_iota(jnp.int32, (bands, length), 0)
    lane = lax.broadcasted_iota(jnp.int32, (bands, length), 1)
    packed = jnp.zeros((bands, length), jnp.float32)
    for n, value in enumerate((norm_own, corr_own, shift_own, sq_own, dot_own)):
        packed = jnp.where(lane == n * bands + line, value, packed)
    own[...] = jnp.sum(packed, axis=0, keepdims=True)
    me = me_y * size_z + me_z

    def tell(t):
        to = (me + t) % count
        return pltpu.make_async_remote_copy(
            src_ref=own, dst_ref=every.at[me], send_sem=sg, recv_sem=qg,
            device_id={"py": to // size_z, "pz": to % size_z}, device_id_type=MESH)

    def tell_start(t, carry):
        tell(t).start()
        return carry
    lax.fori_loop(1, count, tell_start, 0)
    every[me] = own[...]
    free = jnp.zeros((1, length), jnp.float32)

    for n in range(bands):
        free = jnp.where(lane[:1] == n, 1.0 - locked_ref[n].astype(jnp.float32), free)
    every[count] = free
    for sem in (s1, s4):
        await_all(a1.at[:, pl.ds(0, size_y - 1)], sem)
    for sem in (s2, s3):
        await_all(a2.at[:, pl.ds(0, (size_z - 1) * pitch)], sem)
    for sem in (sg, qg):
        await_all(every.at[pl.ds(0, count - 1)], sem)


def finish_kernel(bands, applied_ref, every_ref, out_hbm, rayleigh_hbm, residual_hbm, ray, res, sems):
    copies = [pltpu.make_async_copy(src, dst, sems.at[n]) for n, (src, dst) in enumerate(
        ((applied_ref, out_hbm), (ray, rayleigh_hbm), (res, residual_hbm)))]
    copies[0].start()
    count, _, length = every_ref.shape
    count = count - 1
    table = every_ref[pl.ds(0, count)].reshape(count, length)
    total = jnp.broadcast_to(jnp.sum(table, axis=0, keepdims=True), (8, length))
    used = lax.broadcasted_iota(jnp.int32, (8, length), 1) < bands

    def kind(value, n):
        return pltpu.roll(value, length - n * bands, axis=1)
    norm_sq = jnp.where(used, total, 1.0)
    rayleigh = jnp.where(used, kind(total, 1), 0.0) / norm_sq
    gap = kind(table, 2) - rayleigh[:1]
    residual = kind(table, 3) + gap * (2.0 * kind(table, 4) + gap * table)
    residual = jnp.maximum(jnp.sum(residual, axis=0, keepdims=True), 0.0)
    residual = jnp.sqrt(jnp.where(used, residual, 0.0) / norm_sq)
    ray[...] = rayleigh[:1, :bands]
    res[...] = (residual[:1] * every_ref[count])[:, :bands]
    for copy in copies[1:]:
        copy.start()
    for copy in copies:
        copy.wait()


def two_parts(table):
    table = np.asarray(table, np.float64).astype(np.float32)
    high = table.astype(jnp.bfloat16)
    low = (table - high.astype(np.float32)).astype(jnp.bfloat16)
    return high, low


def exact_matrix(length, inverse):
    counter = np.arange(length)
    angle = 2.0 * math.pi / length * (counter[:, None] * counter[None, :] % length)
    if inverse:
        cosines, sines = np.cos(angle) / length, np.sin(angle) / length
    else:
        cosines, sines = np.cos(angle), -np.sin(angle)
    return np.block([[cosines, sines], [-sines, cosines]])


def fused_hamiltonian(wavefunctions, potential, cutoff_sq, locked_mask, folding, step):
    order, first, plan, masks, square = folding
    _, bands, rows_z, rows_y, length = wavefunctions.shape
    size_y, size_z = lax.axis_size("py"), lax.axis_size("pz")
    slots = bands // size_y
    rows_k = square.shape[0] // size_z
    per = rows_z // step + 1
    units = slots * per
    pitch = 2 * rows_z * rows_k + 8
    count = size_y * size_z
    xf, xi = exact_matrix(length, False), exact_matrix(length, True)
    both_y = np.concatenate([order, order + length])
    order_z = (rows_z * np.arange(size_z)[None, :] + np.arange(rows_z)[:, None]).reshape(-1)
    both_z = np.concatenate([order_z, order_z + length])
    tables = [np.concatenate(two_parts(t), axis=0) for t in (xf, xi)]
    tables += [np.concatenate(two_parts(t), axis=1)
               for t in (xf.T[:, both_z], xi.T[both_z], xf.T[both_y], xi.T[:, both_y])]
    tables = [jnp.asarray(t) for t in tables]
    squares = np.ascontiguousarray(square.reshape(rows_k, size_z, length).swapaxes(0, 1))
    xf_t, xi_t, lf_t, li_t, yf_t, yi_t = tables
    field = wavefunctions.reshape(2, size_y, slots, rows_z, rows_y, length)
    vmem = pl.BlockSpec(memory_space=pltpu.VMEM)
    anywhere = pl.BlockSpec(memory_space=pl.ANY)
    hbm = pl.BlockSpec(memory_space=pltpu.HBM)
    smem = pl.BlockSpec(memory_space=pltpu.SMEM)
    here = pltpu.SemaphoreType.DMA((units,))
    once = pltpu.SemaphoreType.DMA
    f32 = jnp.float32
    in_hbm = functools.partial(pltpu.with_memory_space_constraint, memory_space=pltpu.HBM)
    in_vmem = functools.partial(pltpu.with_memory_space_constraint, memory_space=pltpu.VMEM)
    operands = (xf_t, yf_t, jnp.asarray(masks), lf_t, li_t, jnp.asarray(squares), yi_t, xi_t, potential)
    applied, every = pl.pallas_call(
        functools.partial(main_kernel, size_y, size_z, step, first, plan, WINDOW),
        out_shape=(pltpu.VMEM(field.shape, f32), pltpu.VMEM((count + 1, 1, length), f32)),
        in_specs=[hbm, smem] + [hbm] * (len(operands) + 1),
        out_specs=(vmem, vmem),
        scratch_shapes=[pltpu.VMEM(field.shape, f32), pltpu.SMEM((bands,), jnp.int32)]
        + [pltpu.VMEM(x.shape, x.dtype) for x in operands]
        + [
            pltpu.VMEM(field.shape, f32),
            pltpu.VMEM((2, slots, rows_z, size_y, rows_y, length), f32),
            pltpu.VMEM((slots, size_z * pitch, length), f32),
            pltpu.VMEM((slots, size_z * pitch, length), f32),
            pltpu.VMEM((slots, size_z * pitch, length), f32),
            pltpu.VMEM((5, size_y, slots, per, 8, length), f32),
            pltpu.VMEM((1, length), f32),
            once, here, once, here, once, here, once, here, here,
            pltpu.SemaphoreType.DMA((len(operands) + 1,)), once, once,
        ],
        compiler_params=pltpu.CompilerParams(
            collective_id=0, has_side_effects=True, vmem_limit_bytes=48 * 1024 * 1024),
    )(in_hbm(field), cutoff_sq, *[in_hbm(x) for x in (locked_mask,) + operands])
    out, rayleigh, residual = pl.pallas_call(
        functools.partial(finish_kernel, bands),
        out_shape=(jax.ShapeDtypeStruct(field.shape, f32), jax.ShapeDtypeStruct((1, bands), f32),
                   jax.ShapeDtypeStruct((1, bands), f32)),
        in_specs=[anywhere, vmem],
        out_specs=(hbm, hbm, hbm),
        scratch_shapes=[pltpu.VMEM((1, bands), f32)] * 2 + [pltpu.SemaphoreType.DMA((3,))],
        compiler_params=pltpu.CompilerParams(vmem_limit_bytes=8 * 1024 * 1024),
    )(in_vmem(applied), in_vmem(every))
    return out.reshape(wavefunctions.shape), rayleigh.reshape(bands), residual.reshape(bands)


def gather_kernel(size_y, size_z, own_ref, out_ref, send, recv):
    me_y, me_z = lax.axis_index("py"), lax.axis_index("pz")
    me = me_y * size_z + me_z
    count = size_y * size_z
    barrier = pltpu.get_barrier_semaphore()

    def target(t):
        to = (me + t) % count
        return {"py": to // size_z, "pz": to % size_z}

    def greet(t, carry):
        pl.semaphore_signal(barrier, inc=1, device_id=target(t), device_id_type=MESH)
        return carry
    lax.fori_loop(1, count, greet, 0)
    pl.semaphore_wait(barrier, count - 1)

    def copy(t):
        return pltpu.make_async_remote_copy(
            src_ref=own_ref, dst_ref=out_ref.at[me], send_sem=send.at[t], recv_sem=recv.at[t],
            device_id=target(t), device_id_type=MESH)

    def leave(t, carry):
        copy(t).start()
        return carry
    lax.fori_loop(1, count, leave, 0)
    out_ref[me] = own_ref[...]

    def arrive(t, carry):
        copy(t).wait()
        return carry
    lax.fori_loop(1, count, arrive, 0)


def gather_sums(sums):
    size_y, size_z = lax.axis_size("py"), lax.axis_size("pz")
    count = size_y * size_z
    kinds, bands = sums.shape
    if count > 64:
        return lax.all_gather(sums, ("py", "pz"))
    own = jnp.pad(sums, ((0, 8 - kinds), (0, 128 - bands)))
    vmem = pl.BlockSpec(memory_space=pltpu.VMEM)
    every = pl.pallas_call(
        functools.partial(gather_kernel, size_y, size_z),
        out_shape=jax.ShapeDtypeStruct((count, 8, 128), jnp.float32),
        in_specs=[vmem],
        out_specs=vmem,
        scratch_shapes=[pltpu.SemaphoreType.DMA((count,)), pltpu.SemaphoreType.DMA((count,))],
        compiler_params=pltpu.CompilerParams(collective_id=1, has_side_effects=True),
    )(own)
    return every[:, :kinds, :bands]


def weigh(total, cutoff_sq, length):
    keep = (total <= cutoff_sq[0]).astype(jnp.float32)
    return 0.5 * (math.pi / length) ** 2 * total.astype(jnp.float32) * keep


def plain_kinetic(wavefunctions, kinetic, forward, inverse):
    along_x = "bzyn,kn->bzyk"
    along_y = "bznx,kn->bzkx"
    along_z = "bnyx,kn->bkyx"
    pair = (wavefunctions[0], wavefunctions[1])
    pair = transform(along_x, pair, forward)
    pair = exchange(pair, "py", 0, 2)
    pair = transform(along_y, pair, forward)
    pair = exchange(pair, "pz", 2, 1)
    pair = transform(along_z, pair, forward)
    pair = tuple(part * jnp.swapaxes(kinetic, 0, 1)[None] for part in pair)
    pair = transform(along_z, pair, inverse)
    pair = exchange(pair, "pz", 1, 2)
    pair = transform(along_y, pair, inverse)
    pair = exchange(pair, "py", 2, 0)
    pair = transform(along_x, pair, inverse)
    return jnp.stack(pair)


def body(wavefunctions, potential, cutoff_sq, locked_mask):
    _, bands, rows_z, rows_y, length = wavefunctions.shape
    size_y, size_z = lax.axis_size("py"), lax.axis_size("pz")
    step = 4
    unlocked = 1.0 - locked_mask.astype(jnp.float32)
    fits = size_z == 8 and bands == 8 and length % 128 == 0
    fits = fits and rows_z % step == 0 and rows_z > step and rows_y % 8 == 0
    fits = fits and bands == 2 * size_y
    folding = None
    if fits:
        folding = fold_rows(length, size_z, 3 * size_z) or fold_rows(length, size_z, 2 * size_z)
    if folding is not None:
        return fused_hamiltonian(
            wavefunctions, potential, cutoff_sq, locked_mask, folding, step)
    forward = make_tables(length, False)
    inverse = make_tables(length, True)
    rows = length // size_z
    full_sq = signed_square(jnp.arange(length, dtype=jnp.int32), length)
    own = lax.axis_index("pz") * rows + jnp.arange(rows, dtype=jnp.int32)
    own_sq = signed_square(own, length)
    total = own_sq[:, None, None] + full_sq[None, :, None] + full_sq[None, None, :]
    kinetic = weigh(total, cutoff_sq, length)
    back = plain_kinetic(wavefunctions, kinetic, forward, inverse)
    applied = back + potential[None, None] * wavefunctions
    norm_own = jnp.sum(wavefunctions * wavefunctions, axis=(0, 2, 3, 4))
    corr_own = jnp.sum(wavefunctions * applied, axis=(0, 2, 3, 4))
    shift = jnp.where(norm_own > 0.0, corr_own / jnp.where(norm_own > 0.0, norm_own, 1.0), 0.0)
    rest = applied - shift[None, :, None, None, None] * wavefunctions
    rest_sq = jnp.sum(rest * rest, axis=(0, 2, 3, 4))
    rest_dot = jnp.sum(rest * wavefunctions, axis=(0, 2, 3, 4))
    sums = jnp.stack([norm_own, corr_own, shift, rest_sq, rest_dot])
    every = gather_sums(sums)
    norm_all, corr_all, shift_all, sq_all, dot_all = (every[:, i] for i in range(5))
    norm_sq = jnp.sum(norm_all, axis=0)
    rayleigh = jnp.sum(corr_all, axis=0) / norm_sq
    gap = shift_all - rayleigh[None]
    residual_sq = jnp.sum(sq_all + 2.0 * gap * dot_all + gap * gap * norm_all, axis=0)
    residual_sq = jnp.maximum(residual_sq, 0.0)
    residual_norm = jnp.sqrt(residual_sq / norm_sq) * unlocked
    return (applied, rayleigh, residual_norm)


def solution(mesh):
    in_specs = (P(None, None, "pz", "py", None), P("pz", "py", None), P(), P())
    out_specs = (P(None, None, "pz", "py", None), P(), P())
    return jax.shard_map(body, mesh=mesh, in_specs=in_specs, out_specs=out_specs, check_vma=False)
```

```python
import functools
import math

import jax
import jax.numpy as jnp
import numpy as np
from jax import lax
from jax.experimental import pallas as pl
from jax.experimental.pallas import tpu as pltpu
from jax.sharding import PartitionSpec as P

PREC = lax.Precision.HIGHEST
MESH = pl.DeviceIdType.MESH


def make_tables(length, inverse):
    counter = jnp.arange(length, dtype=jnp.int32)
    phase = counter[:, None] * counter[None, :] % length
    angle = 2.0 * math.pi / length * phase.astype(jnp.float32)
    if inverse:
        return (jnp.cos(angle) / length, jnp.sin(angle) / length)
    return (jnp.cos(angle), -jnp.sin(angle))


def transform(form, pair, tables):
    re, im = pair
    cosines, sines = tables

    def dot(field, table):
        return jnp.einsum(form, field, table, precision=PREC)

    return (dot(re, cosines) - dot(im, sines), dot(re, sines) + dot(im, cosines))


def exchange(pair, axis, split, concat):
    return tuple(
        lax.all_to_all(part, axis, split_axis=split, concat_axis=concat, tiled=True)
        for part in pair
    )


def signed_square(counter, length):
    signed = jnp.where(counter < length // 2, counter, counter - length)
    return signed * signed


def right_matrix(tables):
    cosines, sines = tables
    top = jnp.concatenate([cosines, sines], axis=1)
    return jnp.concatenate([top, jnp.concatenate([-sines, cosines], axis=1)], axis=0)


WINDOW = 2


def fold_rows(length, lanes_of, extra):
    half = length // 2
    group = lanes_of
    reach = {f: math.isqrt(half * half - f * f) for f in range(-half, half)}
    pairs = group // 2
    first_guest = half - extra // 2
    guests = [list(range(first_guest + i, first_guest + i + pairs)) for i in range(0, extra // 2, pairs)]
    hosts = []
    top = first_guest
    while top - pairs > 0 and length - 1 - 2 * reach[top - 1] > 2 and len(hosts) < 8:
        hosts.append(list(range(top - 1, top - 1 - pairs, -1)))
        top -= pairs
    taken = {f for rows in guests + hosts for f in rows}
    plain = [f for f in range(-half, half) if abs(f) not in taken]
    if len(plain) % group or not hosts:
        return None
    hosts = hosts[::-1]
    first = len(plain) // group
    lanes = np.arange(length)
    signed = np.where(lanes < half, lanes, lanes - length)

    def rows_of(groups):
        return [x for rows in groups for f in rows for x in (f, -f)]

    kept_rows = plain + rows_of(hosts)
    order = np.array(kept_rows + rows_of(guests))
    square = np.array(kept_rows)[:, None] ** 2 + signed[None, :] ** 2
    keep = np.ones((len(hosts), group, length), np.float32)
    moves = {}
    for q in range(pairs):
        free = {h: length - 1 - 2 * reach[rows[q]] for h, rows in enumerate(hosts)}
        for g, rows in enumerate(guests):
            f = rows[q]
            at, end = -reach[f], reach[f]
            while at <= end:
                need = end - at + 1
                if not free:
                    return None
                fits = [h for h in free if free[h] >= need]
                h = min(fits, key=lambda h: free[h]) if fits else max(free, key=lambda h: free[h])
                count = min(need, free.pop(h))
                start = reach[hosts[h][q]] + 1
                shift = (start - at) % length
                mask = moves.setdefault((h, g, shift), np.zeros((group, length), np.float32))
                cells = np.arange(start, start + count)
                for e in range(2):
                    mask[2 * q + e, cells] = 1.0
                    keep[h, 2 * q + e, cells] = 0.0
                    square[(first + h) * group + 2 * q + e, cells] = (
                        f * f + np.arange(at, at + count) ** 2)
                at += count
    plan = tuple(sorted(moves))
    masks = np.stack([moves[m] for m in plan] + list(keep))
    return order % length, first, plan, masks, square.astype(np.int32)


def split(field):
    high = field.astype(jnp.bfloat16)
    return high, (field - high.astype(jnp.float32)).astype(jnp.bfloat16)


def left_dot(table_ref, field):
    high, low = split(field)
    size = table_ref.shape[1] // 2
    th, tl = table_ref[:, :size], table_ref[:, size:]
    return jnp.dot(
        jnp.concatenate([th, th, tl], axis=1), jnp.concatenate([high, low, high], axis=0),
        preferred_element_type=jnp.float32)


def right_dot(field, table_ref):
    high, low = split(field)
    size = table_ref.shape[0] // 2
    th, tl = table_ref[:size], table_ref[size:]
    return jnp.dot(
        jnp.concatenate([high, low, high], axis=1), jnp.concatenate([th, th, tl], axis=0),
        preferred_element_type=jnp.float32)


def await_all(ref, sem):
    pltpu.make_async_copy(ref, ref, sem).wait()


def main_kernel(
    size_y, size_z, step, first, plan, window,
    u_hbm, cut_ref, locked_hbm, xf_hbm, yf_hbm, mask_hbm, lf_hbm, li_hbm, sq_hbm, yi_hbm, xi_hbm, pot_hbm,
    o, every,
    u, locked_ref, xf_ref, yf_ref, mask_ref, lf_ref, li_ref, sq_ref, yi_ref, xi_ref, pot_ref,
    a1, r1, a2, r2, r3, r4, sums, own,
    s1, q1, s2, q2, s3, q3, s4, q4, iu, it, sg, qg,
):
    me_y, me_z = lax.axis_index("py"), lax.axis_index("pz")
    _, _, slots, rows_z, rows_y, length = u.shape
    rows_k = sq_ref.shape[1]
    chunks = rows_z // step
    units = slots * chunks + 1
    pitch = a2.shape[1] // size_z
    big = 2 * step * rows_k
    small = big // 2 + 4
    hosts = rows_k - first
    groups = length // size_z - rows_k
    count = size_y * size_z
    bands = size_y * slots

    def is_whole(i, back):
        return i < units - 2 if back else i >= 2

    def place(i, whole, back):
        if whole:
            n = i if back else i - 1
            s, c = n // chunks, n % chunks
            return s, step * c, step, big * c + (0 if back else 8 * (1 - s)), big
        if back:
            n, c = i - (units - 2), chunks - 1
            return slots - 1, step * c + step // 2 * n, step // 2, big * c + small * n, small
        return 0, step // 2 * i, step // 2, small * i, small

    def each(i, act, back):
        if isinstance(i, int):
            act(i, is_whole(i, back))
            return

        @pl.when(is_whole(i, back))
        def _():
            act(i, True)

        @pl.when(jnp.logical_not(is_whole(i, back)))
        def _():
            act(i, False)

    def load(i, whole):
        s, z, n, _, _ = place(i, whole, False)
        zs = pl.ds(z, n)
        return pltpu.make_async_copy(u_hbm.at[:, :, s, zs], u.at[:, :, s, zs], iu.at[i])

    barrier = pltpu.get_barrier_semaphore()
    for d in range(1, size_z):
        pl.semaphore_signal(barrier, inc=1, device_id={"pz": (me_z + d) % size_z}, device_id_type=MESH)
    for d in range(1, size_y):
        pl.semaphore_signal(barrier, inc=1, device_id={"py": (me_y + d) % size_y}, device_id_type=MESH)
    pairs = ((locked_hbm, locked_ref), (xf_hbm, xf_ref), (yf_hbm, yf_ref), (mask_hbm, mask_ref), (lf_hbm, lf_ref), (li_hbm, li_ref),
             (sq_hbm, sq_ref), (yi_hbm, yi_ref), (xi_hbm, xi_ref), (pot_hbm, pot_ref))
    fetches = [pltpu.make_async_copy(src, dst, it.at[n]) for n, (src, dst) in enumerate(pairs)]
    fetches[1].start()
    for i in range(2):
        load(i, False).start()
    for n, fetch in enumerate(fetches):
        if n != 1:
            fetch.start()
    for i in range(2, units):
        load(i, True).start()

    def copy1(i, whole, d):
        s, z, n, _, _ = place(i, whole, False)
        to = (me_y + d) % size_y
        return pltpu.make_async_remote_copy(
            src_ref=a1.at[:, to, s, pl.ds(z, n)], dst_ref=r1.at[:, s, pl.ds(z, n), me_y],
            send_sem=s1, recv_sem=q1.at[i], device_id={"py": to}, device_id_type=MESH)

    def rows_at(m, base, count):
        return pl.ds(pl.multiple_of(m * pitch + base, 8), count)

    def copy2(i, whole, d):
        s, _, _, base, rows = place(i, whole, False)
        to = (me_z + d) % size_z
        return pltpu.make_async_remote_copy(
            src_ref=a2.at[s, rows_at(to, base, rows)], dst_ref=r2.at[s, rows_at(me_z, base, rows)],
            send_sem=s2.at[s], recv_sem=q2.at[i], device_id={"pz": to}, device_id_type=MESH)

    def copy3(i, whole, d):
        s, _, _, base, rows = place(i, whole, True)
        to = (me_z + d) % size_z
        return pltpu.make_async_remote_copy(
            src_ref=r4.at[s, rows_at(to, base, rows)], dst_ref=r3.at[s, rows_at(me_z, base, rows)],
            send_sem=s3.at[s], recv_sem=q3.at[i], device_id={"pz": to}, device_id_type=MESH)

    def copy4(i, whole, d):
        s, z, n, _, _ = place(i, whole, True)
        to = (me_y + d) % size_y
        return pltpu.make_async_remote_copy(
            src_ref=r1.at[:, s, pl.ds(z, n), to], dst_ref=o.at[:, me_y, s, pl.ds(z, n)],
            send_sem=s4, recv_sem=q4.at[i], device_id={"py": to}, device_id_type=MESH)

    order_z = sorted(range(1, size_z), key=lambda d: -min(d, size_z - d))
    order_y = sorted(range(1, size_y), key=lambda d: -min(d, size_y - d))

    def forward_x(i, whole, leave=True):
        s, z, n, _, _ = place(i, whole, False)
        load(i, whole).wait()
        zs = pl.ds(z, n)
        for d in order_y + [0]:
            to = (me_y + d) % size_y
            rows = jnp.concatenate(
                [u[p, to, s, zs].reshape(n * rows_y, length) for p in range(2)], axis=1)
            done = right_dot(rows, xf_ref)
            for p in range(2):
                part = done[:, p * length : (p + 1) * length].reshape(n, rows_y, length)
                if d == 0:
                    r1[p, s, zs, me_y] = part
                else:
                    a1[p, to, s, zs] = part
            if d > 0 and leave:
                copy1(i, whole, d).start()

    def packed(i, whole, back, g, p, z):
        _, _, n, base, _ = place(i, whole, back)
        return base + g * 2 * n + p * n + z

    def forward_y(i, whole):
        s, first_z, n, base, count_rows = place(i, whole, False)
        await_all(a1.at[:, pl.ds(0, size_y - 1), s, pl.ds(first_z, n)], q1.at[i])
        for z in range(0, n, 2):
            sides = []
            for e in range(2):
                sides.append(jnp.concatenate(
                    [r1[p, s, first_z + z + e].reshape(length, length) for p in range(2)], axis=0))
            done = left_dot(yf_ref, jnp.concatenate(sides, axis=1))
            for p in range(2):
                for e in range(2):
                    part = done[p * length : (p + 1) * length, e * length : (e + 1) * length]
                    part = [part[g * size_z : (g + 1) * size_z] for g in range(rows_k + groups)]
                    for h in range(hosts):
                        part[first + h] = part[first + h] * mask_ref[len(plan) + h]
                    for t, (h, g, shift) in enumerate(plan):
                        part[first + h] = part[first + h] + pltpu.roll(
                            part[rows_k + g], shift, axis=1) * mask_ref[t]
                    for g in range(rows_k):
                        a2[s, pl.ds(packed(i, whole, False, g, p, z + e), size_z, stride=pitch)] = part[g]
        r2[s, rows_at(me_z, base, count_rows)] = a2[s, rows_at(me_z, base, count_rows)]

    def leave2(i, whole):
        for d in order_z:
            copy2(i, whole, d).start()

    def arrive2(i, whole):
        await_all(a2.at[0, pl.ds(0, (size_z - 1) * place(i, whole, False)[4])], q2.at[i])

    def leave3(i, whole):
        for d in order_z:
            copy3(i, whole, d).start()

    def arrive3(i, whole):
        await_all(a2.at[0, pl.ds(0, (size_z - 1) * place(i, whole, True)[4])], q3.at[i])

    kz = lax.broadcasted_iota(jnp.int32, (length, length), 0)
    kz_sq = signed_square(kz, length)

    def z_rows(s, ks):
        spots = [[], []]
        for back in range(2):
            for i in range(units):
                whole = is_whole(i, back)
                if place(i, whole, back)[0] == s:
                    spots[back] += [(i, whole, z) for z in range(place(i, whole, back)[2])]

        def at(k, p, n, back):
            i, whole, z = spots[back][n]
            return pl.ds(packed(i, whole, back, k, p, z), size_z, stride=pitch)
        sides, weights = [], []
        for k in ks:
            sides.append(jnp.concatenate(
                [r2[s, at(k, p, n, 0)] for p in range(2) for n in range(rows_z)], axis=0))
            weights.append(weigh(kz_sq + sq_ref[me_z, pl.ds(k, 1)], cut_ref, length))
        weight = jnp.concatenate(weights, axis=1)
        spectrum = left_dot(lf_ref, jnp.concatenate(sides, axis=1))
        done = left_dot(li_ref, spectrum * jnp.concatenate([weight, weight], axis=0))
        for e, k in enumerate(ks):
            for p in range(2):
                for n in range(rows_z):
                    top = p * length + n * size_z
                    r4[s, at(k, p, n, 1)] = done[top : top + size_z, e * length : (e + 1) * length]

    def both_z(s):
        def two_rows(h, carry):
            z_rows(s, (2 * h, 2 * h + 1))
            return carry
        lax.fori_loop(0, rows_k // 2, two_rows, 0)
        if rows_k % 2:
            z_rows(s, (rows_k - 1,))
        r3[s, rows_at(me_z, 0, pitch)] = r4[s, rows_at(me_z, 0, pitch)]

    def inverse_y(i, whole):
        s, first_z, n, _, _ = place(i, whole, True)
        for z in range(0, n, 2):
            sides = []
            for e in range(2):
                both = []
                for p in range(2):
                    part = [r3[s, pl.ds(packed(i, whole, True, g, p, z + e), size_z, stride=pitch)]
                            for g in range(rows_k)]
                    guests = [None] * groups
                    for t, (h, g, shift) in enumerate(plan):
                        moved = pltpu.roll(part[first + h] * mask_ref[t], length - shift, axis=1)
                        guests[g] = moved if guests[g] is None else guests[g] + moved
                    for h in range(hosts):
                        part[first + h] = part[first + h] * mask_ref[len(plan) + h]
                    both += part + guests
                sides.append(jnp.concatenate(both, axis=0))
            done = left_dot(yi_ref, jnp.concatenate(sides, axis=1))
            for p in range(2):
                for e in range(2):
                    part = done[p * length : (p + 1) * length, e * length : (e + 1) * length]
                    r1[p, s, first_z + z + e] = part.reshape(size_y, rows_y, length)
        for d in order_y:
            copy4(i, whole, d).start()
        zs = pl.ds(first_z, n)
        o[:, me_y, s, zs] = r1[:, s, zs, me_y]

    def inverse_x(i, whole):
        s, z, n, _, _ = place(i, whole, True)
        zs = pl.ds(z, n)
        area = n * rows_y
        pot = pot_ref[zs].reshape(area, length)
        await_all(a1.at[:, pl.ds(0, size_y - 1), s, zs], q4.at[i])
        for d in range(size_y):
            owner = (me_y + size_y - d) % size_y
            rows = jnp.concatenate(
                [o[p, owner, s, zs].reshape(area, length) for p in range(2)], axis=1)
            done = right_dot(rows, xi_ref)
            fields, results = [], []
            for p in range(2):
                field = u[p, owner, s, zs].reshape(area, length)
                part = done[:, p * length : (p + 1) * length] + pot * field
                o[p, owner, s, zs] = part.reshape(n, rows_y, length)
                fields.append(field.reshape(area // 8, 8, length))
                results.append(part.reshape(area // 8, 8, length))

            def total(values):
                return jnp.sum(values[0] + values[1], axis=0)
            norm = total([f * f for f in fields])
            corr = total([f * r for f, r in zip(fields, results)])
            shift = jnp.where(norm > 0.0, corr / jnp.where(norm > 0.0, norm, 1.0), 0.0)
            gaps = [r - shift[None] * f for f, r in zip(fields, results)]
            values = (norm, corr, shift, total([g * g for g in gaps]),
                      total([g * f for g, f in zip(gaps, fields)]))
            for k, value in enumerate(values):
                sums[k, owner, s, z // step if whole else z // (step // 2) - (chunks - 1)] = value

    sums[:, :, :, chunks] = jnp.zeros((5, size_y, slots, 8, length), jnp.float32)
    fetches[1].wait()

    def before(i, carry):
        forward_x(i, False, False)
        return carry
    lax.fori_loop(0, 2, before, 0)
    pl.semaphore_wait(barrier, size_y + size_z - 2)
    for i in range(2):
        for d in order_y:
            copy1(i, False, d).start()
    for n, fetch in enumerate(fetches):
        if n != 1:
            fetch.wait()

    def outward(i, carry):
        @pl.when(i + 2 < units)
        def _():
            each(i + 2, forward_x, False)
        each(i, forward_y, False)

        @pl.when(i >= window)
        def _():
            each(i - window, arrive2, False)
        each(i, leave2, False)

        @pl.when(i == chunks + window)
        def _():
            both_z(0)
        return carry
    lax.fori_loop(0, units, outward, 0)

    def homeward(i, carry):
        @pl.when(i < window)
        def _():
            each(units - window + i, arrive2, False)

        @pl.when(i >= window)
        def _():
            each(i - window, arrive3, True)

        @pl.when(i < units)
        def _():
            each(i, leave3, True)

        @pl.when(i == window - 1)
        def _():
            both_z(1)

        @pl.when(i >= window)
        def _():
            each(i - window, inverse_y, True)

        @pl.when(i > window + 1)
        def _():
            each(i - window - 2, inverse_x, True)
        return carry
    lax.fori_loop(0, units + window, homeward, 0)
    for i in range(units - 2, units):
        inverse_x(i, False)

    norm, corr, shift, rest_sq, rest_dot = (
        sums[n].reshape(bands, (chunks + 1) * 8, length) for n in range(5))

    def of_band(value):
        return jnp.sum(jnp.sum(value, axis=1), axis=1, keepdims=True)
    norm_own, corr_own = of_band(norm), of_band(corr)
    shift_own = jnp.where(norm_own > 0.0, corr_own / jnp.where(norm_own > 0.0, norm_own, 1.0), 0.0)
    gap = shift - shift_own[:, :, None]
    sq_own = of_band(rest_sq + gap * (2.0 * rest_dot + gap * norm))
    dot_own = of_band(rest_dot + gap * norm)
    line = lax.broadcasted_iota(jnp.int32, (bands, length), 0)
    lane = lax.broadcasted_iota(jnp.int32, (bands, length), 1)
    packed = jnp.zeros((bands, length), jnp.float32)
    for n, value in enumerate((norm_own, corr_own, shift_own, sq_own, dot_own)):
        packed = jnp.where(lane == n * bands + line, value, packed)
    own[...] = jnp.sum(packed, axis=0, keepdims=True)
    me = me_y * size_z + me_z

    def tell(t):
        to = (me + t) % count
        return pltpu.make_async_remote_copy(
            src_ref=own, dst_ref=every.at[me], send_sem=sg, recv_sem=qg,
            device_id={"py": to // size_z, "pz": to % size_z}, device_id_type=MESH)

    def tell_start(t, carry):
        tell(t).start()
        return carry
    lax.fori_loop(1, count, tell_start, 0)
    every[me] = own[...]
    free = jnp.zeros((1, length), jnp.float32)

    for n in range(bands):
        free = jnp.where(lane[:1] == n, 1.0 - locked_ref[n].astype(jnp.float32), free)
    every[count] = free
    for sem in (s1, s4):
        await_all(a1.at[:, pl.ds(0, size_y - 1)], sem)
    for s in range(slots):
        for sem, extra in ((s2, 8 * (s == 0)), (s3, 8 * (s == slots - 1))):
            await_all(a2.at[0, pl.ds(0, (size_z - 1) * (chunks * big + extra))], sem.at[s])
    for sem in (sg, qg):
        await_all(every.at[pl.ds(0, count - 1)], sem)


def finish_kernel(bands, applied_ref, every_ref, out_hbm, rayleigh_hbm, residual_hbm, ray, res, sems):
    copies = [pltpu.make_async_copy(src, dst, sems.at[n]) for n, (src, dst) in enumerate(
        ((applied_ref, out_hbm), (ray, rayleigh_hbm), (res, residual_hbm)))]
    copies[0].start()
    count, _, length = every_ref.shape
    count = count - 1
    table = every_ref[pl.ds(0, count)].reshape(count, length)
    total = jnp.broadcast_to(jnp.sum(table, axis=0, keepdims=True), (8, length))
    used = lax.broadcasted_iota(jnp.int32, (8, length), 1) < bands

    def kind(value, n):
        return pltpu.roll(value, length - n * bands, axis=1)
    norm_sq = jnp.where(used, total, 1.0)
    rayleigh = jnp.where(used, kind(total, 1), 0.0) / norm_sq
    gap = kind(table, 2) - rayleigh[:1]
    residual = kind(table, 3) + gap * (2.0 * kind(table, 4) + gap * table)
    residual = jnp.maximum(jnp.sum(residual, axis=0, keepdims=True), 0.0)
    residual = jnp.sqrt(jnp.where(used, residual, 0.0) / norm_sq)
    ray[...] = rayleigh[:1, :bands]
    res[...] = (residual[:1] * every_ref[count])[:, :bands]
    for copy in copies[1:]:
        copy.start()
    for copy in copies:
        copy.wait()


def two_parts(table):
    table = np.asarray(table, np.float64).astype(np.float32)
    high = table.astype(jnp.bfloat16)
    low = (table - high.astype(np.float32)).astype(jnp.bfloat16)
    return high, low


def exact_matrix(length, inverse):
    counter = np.arange(length)
    angle = 2.0 * math.pi / length * (counter[:, None] * counter[None, :] % length)
    if inverse:
        cosines, sines = np.cos(angle) / length, np.sin(angle) / length
    else:
        cosines, sines = np.cos(angle), -np.sin(angle)
    return np.block([[cosines, sines], [-sines, cosines]])


def fused_hamiltonian(wavefunctions, potential, cutoff_sq, locked_mask, folding, step):
    order, first, plan, masks, square = folding
    _, bands, rows_z, rows_y, length = wavefunctions.shape
    size_y, size_z = lax.axis_size("py"), lax.axis_size("pz")
    slots = bands // size_y
    rows_k = square.shape[0] // size_z
    chunks = rows_z // step
    units = slots * chunks + 1
    pitch = 2 * rows_z * rows_k + 8
    count = size_y * size_z
    xf, xi = exact_matrix(length, False), exact_matrix(length, True)
    both_y = np.concatenate([order, order + length])
    order_z = (rows_z * np.arange(size_z)[None, :] + np.arange(rows_z)[:, None]).reshape(-1)
    both_z = np.concatenate([order_z, order_z + length])
    tables = [np.concatenate(two_parts(t), axis=0) for t in (xf, xi)]
    tables += [np.concatenate(two_parts(t), axis=1)
               for t in (xf.T[:, both_z], xi.T[both_z], xf.T[both_y], xi.T[:, both_y])]
    tables = [jnp.asarray(t) for t in tables]
    squares = np.ascontiguousarray(square.reshape(rows_k, size_z, length).swapaxes(0, 1))
    xf_t, xi_t, lf_t, li_t, yf_t, yi_t = tables
    field = wavefunctions.reshape(2, size_y, slots, rows_z, rows_y, length)
    vmem = pl.BlockSpec(memory_space=pltpu.VMEM)
    anywhere = pl.BlockSpec(memory_space=pl.ANY)
    hbm = pl.BlockSpec(memory_space=pltpu.HBM)
    smem = pl.BlockSpec(memory_space=pltpu.SMEM)
    here = pltpu.SemaphoreType.DMA((units,))
    once = pltpu.SemaphoreType.DMA
    both = pltpu.SemaphoreType.DMA((slots,))
    f32 = jnp.float32
    in_hbm = functools.partial(pltpu.with_memory_space_constraint, memory_space=pltpu.HBM)
    in_vmem = functools.partial(pltpu.with_memory_space_constraint, memory_space=pltpu.VMEM)
    operands = (xf_t, yf_t, jnp.asarray(masks), lf_t, li_t, jnp.asarray(squares), yi_t, xi_t, potential)
    applied, every = pl.pallas_call(
        functools.partial(main_kernel, size_y, size_z, step, first, plan, WINDOW),
        out_shape=(pltpu.VMEM(field.shape, f32), pltpu.VMEM((count + 1, 1, length), f32)),
        in_specs=[hbm, smem] + [hbm] * (len(operands) + 1),
        out_specs=(vmem, vmem),
        scratch_shapes=[pltpu.VMEM(field.shape, f32), pltpu.SMEM((bands,), jnp.int32)]
        + [pltpu.VMEM(x.shape, x.dtype) for x in operands]
        + [
            pltpu.VMEM(field.shape, f32),
            pltpu.VMEM((2, slots, rows_z, size_y, rows_y, length), f32),
            pltpu.VMEM((slots, size_z * pitch, length), f32),
            pltpu.VMEM((slots, size_z * pitch, length), f32),
            pltpu.VMEM((slots, size_z * pitch, length), f32),
            pltpu.VMEM((slots, size_z * pitch, length), f32),
            pltpu.VMEM((5, size_y, slots, chunks + 1, 8, length), f32),
            pltpu.VMEM((1, length), f32),
            once, here, both, here, both, here, once, here, here,
            pltpu.SemaphoreType.DMA((len(operands) + 1,)), once, once,
        ],
        compiler_params=pltpu.CompilerParams(
            collective_id=0, has_side_effects=True, vmem_limit_bytes=48 * 1024 * 1024),
    )(in_hbm(field), cutoff_sq, *[in_hbm(x) for x in (locked_mask,) + operands])
    out, rayleigh, residual = pl.pallas_call(
        functools.partial(finish_kernel, bands),
        out_shape=(jax.ShapeDtypeStruct(field.shape, f32), jax.ShapeDtypeStruct((1, bands), f32),
                   jax.ShapeDtypeStruct((1, bands), f32)),
        in_specs=[anywhere, vmem],
        out_specs=(hbm, hbm, hbm),
        scratch_shapes=[pltpu.VMEM((1, bands), f32)] * 2 + [pltpu.SemaphoreType.DMA((3,))],
        compiler_params=pltpu.CompilerParams(vmem_limit_bytes=8 * 1024 * 1024),
    )(in_vmem(applied), in_vmem(every))
    return out.reshape(wavefunctions.shape), rayleigh.reshape(bands), residual.reshape(bands)


def gather_kernel(size_y, size_z, own_ref, out_ref, send, recv):
    me_y, me_z = lax.axis_index("py"), lax.axis_index("pz")
    me = me_y * size_z + me_z
    count = size_y * size_z
    barrier = pltpu.get_barrier_semaphore()

    def target(t):
        to = (me + t) % count
        return {"py": to // size_z, "pz": to % size_z}

    def greet(t, carry):
        pl.semaphore_signal(barrier, inc=1, device_id=target(t), device_id_type=MESH)
        return carry
    lax.fori_loop(1, count, greet, 0)
    pl.semaphore_wait(barrier, count - 1)

    def copy(t):
        return pltpu.make_async_remote_copy(
            src_ref=own_ref, dst_ref=out_ref.at[me], send_sem=send.at[t], recv_sem=recv.at[t],
            device_id=target(t), device_id_type=MESH)

    def leave(t, carry):
        copy(t).start()
        return carry
    lax.fori_loop(1, count, leave, 0)
    out_ref[me] = own_ref[...]

    def arrive(t, carry):
        copy(t).wait()
        return carry
    lax.fori_loop(1, count, arrive, 0)


def gather_sums(sums):
    size_y, size_z = lax.axis_size("py"), lax.axis_size("pz")
    count = size_y * size_z
    kinds, bands = sums.shape
    if count > 64:
        return lax.all_gather(sums, ("py", "pz"))
    own = jnp.pad(sums, ((0, 8 - kinds), (0, 128 - bands)))
    vmem = pl.BlockSpec(memory_space=pltpu.VMEM)
    every = pl.pallas_call(
        functools.partial(gather_kernel, size_y, size_z),
        out_shape=jax.ShapeDtypeStruct((count, 8, 128), jnp.float32),
        in_specs=[vmem],
        out_specs=vmem,
        scratch_shapes=[pltpu.SemaphoreType.DMA((count,)), pltpu.SemaphoreType.DMA((count,))],
        compiler_params=pltpu.CompilerParams(collective_id=1, has_side_effects=True),
    )(own)
    return every[:, :kinds, :bands]


def weigh(total, cutoff_sq, length):
    keep = (total <= cutoff_sq[0]).astype(jnp.float32)
    return 0.5 * (math.pi / length) ** 2 * total.astype(jnp.float32) * keep


def plain_kinetic(wavefunctions, kinetic, forward, inverse):
    along_x = "bzyn,kn->bzyk"
    along_y = "bznx,kn->bzkx"
    along_z = "bnyx,kn->bkyx"
    pair = (wavefunctions[0], wavefunctions[1])
    pair = transform(along_x, pair, forward)
    pair = exchange(pair, "py", 0, 2)
    pair = transform(along_y, pair, forward)
    pair = exchange(pair, "pz", 2, 1)
    pair = transform(along_z, pair, forward)
    pair = tuple(part * jnp.swapaxes(kinetic, 0, 1)[None] for part in pair)
    pair = transform(along_z, pair, inverse)
    pair = exchange(pair, "pz", 1, 2)
    pair = transform(along_y, pair, inverse)
    pair = exchange(pair, "py", 2, 0)
    pair = transform(along_x, pair, inverse)
    return jnp.stack(pair)


def body(wavefunctions, potential, cutoff_sq, locked_mask):
    _, bands, rows_z, rows_y, length = wavefunctions.shape
    size_y, size_z = lax.axis_size("py"), lax.axis_size("pz")
    step = 4
    unlocked = 1.0 - locked_mask.astype(jnp.float32)
    fits = size_z == 8 and bands == 8 and length % 128 == 0
    fits = fits and rows_z % step == 0 and rows_z > step and rows_y % 8 == 0
    fits = fits and bands == 2 * size_y
    folding = None
    if fits:
        folding = fold_rows(length, size_z, 3 * size_z) or fold_rows(length, size_z, 2 * size_z)
    if folding is not None:
        return fused_hamiltonian(
            wavefunctions, potential, cutoff_sq, locked_mask, folding, step)
    forward = make_tables(length, False)
    inverse = make_tables(length, True)
    rows = length // size_z
    full_sq = signed_square(jnp.arange(length, dtype=jnp.int32), length)
    own = lax.axis_index("pz") * rows + jnp.arange(rows, dtype=jnp.int32)
    own_sq = signed_square(own, length)
    total = own_sq[:, None, None] + full_sq[None, :, None] + full_sq[None, None, :]
    kinetic = weigh(total, cutoff_sq, length)
    back = plain_kinetic(wavefunctions, kinetic, forward, inverse)
    applied = back + potential[None, None] * wavefunctions
    norm_own = jnp.sum(wavefunctions * wavefunctions, axis=(0, 2, 3, 4))
    corr_own = jnp.sum(wavefunctions * applied, axis=(0, 2, 3, 4))
    shift = jnp.where(norm_own > 0.0, corr_own / jnp.where(norm_own > 0.0, norm_own, 1.0), 0.0)
    rest = applied - shift[None, :, None, None, None] * wavefunctions
    rest_sq = jnp.sum(rest * rest, axis=(0, 2, 3, 4))
    rest_dot = jnp.sum(rest * wavefunctions, axis=(0, 2, 3, 4))
    sums = jnp.stack([norm_own, corr_own, shift, rest_sq, rest_dot])
    every = gather_sums(sums)
    norm_all, corr_all, shift_all, sq_all, dot_all = (every[:, i] for i in range(5))
    norm_sq = jnp.sum(norm_all, axis=0)
    rayleigh = jnp.sum(corr_all, axis=0) / norm_sq
    gap = shift_all - rayleigh[None]
    residual_sq = jnp.sum(sq_all + 2.0 * gap * dot_all + gap * gap * norm_all, axis=0)
    residual_sq = jnp.maximum(residual_sq, 0.0)
    residual_norm = jnp.sqrt(residual_sq / norm_sq) * unlocked
    return (applied, rayleigh, residual_norm)


def solution(mesh):
    in_specs = (P(None, None, "pz", "py", None), P("pz", "py", None), P(), P())
    out_specs = (P(None, None, "pz", "py", None), P(), P())
    return jax.shard_map(body, mesh=mesh, in_specs=in_specs, out_specs=out_specs, check_vma=False)
```

```python
import functools
import math

import jax
import jax.numpy as jnp
import numpy as np
from jax import lax
from jax.experimental import pallas as pl
from jax.experimental.pallas import tpu as pltpu
from jax.sharding import PartitionSpec as P

PREC = lax.Precision.HIGHEST
MESH = pl.DeviceIdType.MESH


def make_tables(length, inverse):
    counter = jnp.arange(length, dtype=jnp.int32)
    phase = counter[:, None] * counter[None, :] % length
    angle = 2.0 * math.pi / length * phase.astype(jnp.float32)
    if inverse:
        return (jnp.cos(angle) / length, jnp.sin(angle) / length)
    return (jnp.cos(angle), -jnp.sin(angle))


def transform(form, pair, tables):
    re, im = pair
    cosines, sines = tables

    def dot(field, table):
        return jnp.einsum(form, field, table, precision=PREC)

    return (dot(re, cosines) - dot(im, sines), dot(re, sines) + dot(im, cosines))


def exchange(pair, axis, split, concat):
    return tuple(
        lax.all_to_all(part, axis, split_axis=split, concat_axis=concat, tiled=True)
        for part in pair
    )


def signed_square(counter, length):
    signed = jnp.where(counter < length // 2, counter, counter - length)
    return signed * signed


def right_matrix(tables):
    cosines, sines = tables
    top = jnp.concatenate([cosines, sines], axis=1)
    return jnp.concatenate([top, jnp.concatenate([-sines, cosines], axis=1)], axis=0)


WINDOW = 2


def fold_rows(length, lanes_of, extra):
    half = length // 2
    group = lanes_of
    reach = {f: math.isqrt(half * half - f * f) for f in range(-half, half)}
    pairs = group // 2
    first_guest = half - extra // 2
    guests = [list(range(first_guest + i, first_guest + i + pairs)) for i in range(0, extra // 2, pairs)]
    hosts = []
    top = first_guest
    while top - pairs > 0 and length - 1 - 2 * reach[top - 1] > 2 and len(hosts) < 8:
        hosts.append(list(range(top - 1, top - 1 - pairs, -1)))
        top -= pairs
    taken = {f for rows in guests + hosts for f in rows}
    plain = [f for f in range(-half, half) if abs(f) not in taken]
    if len(plain) % group or not hosts:
        return None
    hosts = hosts[::-1]
    first = len(plain) // group
    lanes = np.arange(length)
    signed = np.where(lanes < half, lanes, lanes - length)

    def rows_of(groups):
        return [x for rows in groups for f in rows for x in (f, -f)]

    kept_rows = plain + rows_of(hosts)
    order = np.array(kept_rows + rows_of(guests))
    square = np.array(kept_rows)[:, None] ** 2 + signed[None, :] ** 2
    keep = np.ones((len(hosts), group, length), np.float32)
    moves = {}
    for q in range(pairs):
        free = {h: length - 1 - 2 * reach[rows[q]] for h, rows in enumerate(hosts)}
        for g, rows in enumerate(guests):
            f = rows[q]
            at, end = -reach[f], reach[f]
            while at <= end:
                need = end - at + 1
                if not free:
                    return None
                fits = [h for h in free if free[h] >= need]
                h = min(fits, key=lambda h: free[h]) if fits else max(free, key=lambda h: free[h])
                count = min(need, free.pop(h))
                start = reach[hosts[h][q]] + 1
                shift = (start - at) % length
                mask = moves.setdefault((h, g, shift), np.zeros((group, length), np.float32))
                cells = np.arange(start, start + count)
                for e in range(2):
                    mask[2 * q + e, cells] = 1.0
                    keep[h, 2 * q + e, cells] = 0.0
                    square[(first + h) * group + 2 * q + e, cells] = (
                        f * f + np.arange(at, at + count) ** 2)
                at += count
    plan = tuple(sorted(moves))
    masks = np.stack([moves[m] for m in plan] + list(keep))
    return order % length, first, plan, masks, square.astype(np.int32)


def split(field):
    high = field.astype(jnp.bfloat16)
    return high, (field - high.astype(jnp.float32)).astype(jnp.bfloat16)


def left_dot(table_ref, field):
    high, low = split(field)
    size = table_ref.shape[1] // 2
    th, tl = table_ref[:, :size], table_ref[:, size:]
    return jnp.dot(
        jnp.concatenate([th, th, tl], axis=1), jnp.concatenate([high, low, high], axis=0),
        preferred_element_type=jnp.float32)


def right_dot(field, table_ref):
    high, low = split(field)
    size = table_ref.shape[0] // 2
    th, tl = table_ref[:size], table_ref[size:]
    return jnp.dot(
        jnp.concatenate([high, low, high], axis=1), jnp.concatenate([th, th, tl], axis=0),
        preferred_element_type=jnp.float32)


def await_all(ref, sem):
    pltpu.make_async_copy(ref, ref, sem).wait()


def main_kernel(
    size_y, size_z, step, first, plan, window,
    u_hbm, cut_ref, locked_hbm, xf_hbm, yf_hbm, mask_hbm, lf_hbm, li_hbm, sq_hbm, yi_hbm, xi_hbm, pot_hbm,
    o, every,
    u, locked_ref, xf_ref, yf_ref, mask_ref, lf_ref, li_ref, sq_ref, yi_ref, xi_ref, pot_ref,
    a1, r1, a2, r2, r3, r4, sums, own,
    s1, q1, s2, q2, s3, q3, s4, q4, iu, it, sg, qg,
):
    me_y, me_z = lax.axis_index("py"), lax.axis_index("pz")
    _, _, slots, rows_z, rows_y, length = u.shape
    rows_k = sq_ref.shape[1]
    chunks = rows_z // step
    units = slots * chunks + 1
    pitch = a2.shape[1] // size_z
    big = 2 * step * rows_k
    small = big // 2 + 4
    hosts = rows_k - first
    groups = length // size_z - rows_k
    count = size_y * size_z
    bands = size_y * slots

    def is_whole(i, back):
        return i < units - 2 if back else i >= 2

    def place(i, whole, back):
        if whole:
            n = i if back else i - 1
            s, c = n // chunks, n % chunks
            return s, step * c, step, big * c + (0 if back else 8 * (1 - s)), big
        if back:
            n, c = i - (units - 2), chunks - 1
            return slots - 1, step * c + step // 2 * n, step // 2, big * c + small * n, small
        return 0, step // 2 * i, step // 2, small * i, small

    def each(i, act, back):
        if isinstance(i, int):
            act(i, is_whole(i, back))
            return

        @pl.when(is_whole(i, back))
        def _():
            act(i, True)

        @pl.when(jnp.logical_not(is_whole(i, back)))
        def _():
            act(i, False)

    def load(i, whole):
        s, z, n, _, _ = place(i, whole, False)
        zs = pl.ds(z, n)
        return pltpu.make_async_copy(u_hbm.at[:, :, s, zs], u.at[:, :, s, zs], iu.at[i])

    barrier = pltpu.get_barrier_semaphore()
    for d in range(1, size_z):
        pl.semaphore_signal(barrier, inc=1, device_id={"pz": (me_z + d) % size_z}, device_id_type=MESH)
    for d in range(1, size_y):
        pl.semaphore_signal(barrier, inc=1, device_id={"py": (me_y + d) % size_y}, device_id_type=MESH)
    pairs = ((locked_hbm, locked_ref), (xf_hbm, xf_ref), (yf_hbm, yf_ref), (mask_hbm, mask_ref), (lf_hbm, lf_ref), (li_hbm, li_ref),
             (sq_hbm, sq_ref), (yi_hbm, yi_ref), (xi_hbm, xi_ref), (pot_hbm, pot_ref))
    fetches = [pltpu.make_async_copy(src, dst, it.at[n]) for n, (src, dst) in enumerate(pairs)]
    fetches[1].start()
    for i in range(2):
        load(i, False).start()
    for n, fetch in enumerate(fetches):
        if n != 1:
            fetch.start()
    for i in range(2, units):
        load(i, True).start()

    def copy1(i, whole, d):
        s, z, n, _, _ = place(i, whole, False)
        to = (me_y + d) % size_y
        return pltpu.make_async_remote_copy(
            src_ref=a1.at[:, to, s, pl.ds(z, n)], dst_ref=r1.at[:, s, pl.ds(z, n), me_y],
            send_sem=s1, recv_sem=q1.at[i], device_id={"py": to}, device_id_type=MESH)

    def rows_at(m, base, count):
        return pl.ds(pl.multiple_of(m * pitch + base, 8), count)

    def copy2(i, whole, d):
        s, _, _, base, rows = place(i, whole, False)
        to = (me_z + d) % size_z
        return pltpu.make_async_remote_copy(
            src_ref=a2.at[s, rows_at(to, base, rows)], dst_ref=r2.at[s, rows_at(me_z, base, rows)],
            send_sem=s2.at[s], recv_sem=q2.at[i], device_id={"pz": to}, device_id_type=MESH)

    def copy3(i, whole, d):
        s, _, _, base, rows = place(i, whole, True)
        to = (me_z + d) % size_z
        return pltpu.make_async_remote_copy(
            src_ref=r4.at[s, rows_at(to, base, rows)], dst_ref=r3.at[s, rows_at(me_z, base, rows)],
            send_sem=s3.at[s], recv_sem=q3.at[i], device_id={"pz": to}, device_id_type=MESH)

    def copy4(i, whole, d):
        s, z, n, _, _ = place(i, whole, True)
        to = (me_y + d) % size_y
        return pltpu.make_async_remote_copy(
            src_ref=r1.at[:, s, pl.ds(z, n), to], dst_ref=o.at[:, me_y, s, pl.ds(z, n)],
            send_sem=s4, recv_sem=q4.at[i], device_id={"py": to}, device_id_type=MESH)

    order_z = sorted(range(1, size_z), key=lambda d: -min(d, size_z - d))
    order_y = sorted(range(1, size_y), key=lambda d: -min(d, size_y - d))

    def forward_x(i, whole, leave=True):
        s, z, n, _, _ = place(i, whole, False)
        load(i, whole).wait()
        zs = pl.ds(z, n)
        for d in order_y + [0]:
            to = (me_y + d) % size_y
            rows = jnp.concatenate(
                [u[p, to, s, zs].reshape(n * rows_y, length) for p in range(2)], axis=1)
            done = right_dot(rows, xf_ref)
            for p in range(2):
                part = done[:, p * length : (p + 1) * length].reshape(n, rows_y, length)
                if d == 0:
                    r1[p, s, zs, me_y] = part
                else:
                    a1[p, to, s, zs] = part
            if d > 0 and leave:
                copy1(i, whole, d).start()

    def packed(i, whole, back, g, p, z):
        _, _, n, base, _ = place(i, whole, back)
        return base + g * 2 * n + p * n + z

    def forward_y(i, whole):
        s, first_z, n, base, count_rows = place(i, whole, False)
        await_all(a1.at[:, pl.ds(0, size_y - 1), s, pl.ds(first_z, n)], q1.at[i])
        for z in range(0, n, 2):
            sides = []
            for e in range(2):
                sides.append(jnp.concatenate(
                    [r1[p, s, first_z + z + e].reshape(length, length) for p in range(2)], axis=0))
            done = left_dot(yf_ref, jnp.concatenate(sides, axis=1))
            for p in range(2):
                for e in range(2):
                    part = done[p * length : (p + 1) * length, e * length : (e + 1) * length]
                    part = [part[g * size_z : (g + 1) * size_z] for g in range(rows_k + groups)]
                    for h in range(hosts):
                        part[first + h] = part[first + h] * mask_ref[len(plan) + h]
                    for t, (h, g, shift) in enumerate(plan):
                        part[first + h] = part[first + h] + pltpu.roll(
                            part[rows_k + g], shift, axis=1) * mask_ref[t]
                    for g in range(rows_k):
                        a2[s, pl.ds(packed(i, whole, False, g, p, z + e), size_z, stride=pitch)] = part[g]
        r2[s, rows_at(me_z, base, count_rows)] = a2[s, rows_at(me_z, base, count_rows)]

    def leave2(i, whole):
        for d in order_z:
            copy2(i, whole, d).start()

    def arrive2(i, whole):
        await_all(a2.at[0, pl.ds(0, (size_z - 1) * place(i, whole, False)[4])], q2.at[i])

    def leave3(i, whole):
        for d in order_z:
            copy3(i, whole, d).start()

    def arrive3(i, whole):
        await_all(a2.at[0, pl.ds(0, (size_z - 1) * place(i, whole, True)[4])], q3.at[i])

    kz = lax.broadcasted_iota(jnp.int32, (length, length), 0)
    kz_sq = signed_square(kz, length)

    def z_rows(s, ks):
        spots = [[], []]
        for back in range(2):
            for i in range(units):
                whole = is_whole(i, back)
                if place(i, whole, back)[0] == s:
                    spots[back] += [(i, whole, z) for z in range(place(i, whole, back)[2])]

        def at(k, p, n, back):
            i, whole, z = spots[back][n]
            return pl.ds(packed(i, whole, back, k, p, z), size_z, stride=pitch)
        sides, weights = [], []
        for k in ks:
            sides.append(jnp.concatenate(
                [r2[s, at(k, p, n, 0)] for p in range(2) for n in range(rows_z)], axis=0))
            weights.append(weigh(kz_sq + sq_ref[me_z, pl.ds(k, 1)], cut_ref, length))
        weight = jnp.concatenate(weights, axis=1)
        spectrum = left_dot(lf_ref, jnp.concatenate(sides, axis=1))
        done = left_dot(li_ref, spectrum * jnp.concatenate([weight, weight], axis=0))
        for e, k in enumerate(ks):
            for p in range(2):
                for n in range(rows_z):
                    top = p * length + n * size_z
                    r4[s, at(k, p, n, 1)] = done[top : top + size_z, e * length : (e + 1) * length]

    def both_z(s):
        def two_rows(h, carry):
            z_rows(s, (2 * h, 2 * h + 1))
            return carry
        lax.fori_loop(0, rows_k // 2, two_rows, 0)
        if rows_k % 2:
            z_rows(s, (rows_k - 1,))
        r3[s, rows_at(me_z, 0, pitch)] = r4[s, rows_at(me_z, 0, pitch)]

    def inverse_y(i, whole):
        s, first_z, n, _, _ = place(i, whole, True)
        for z in range(0, n, 2):
            sides = []
            for e in range(2):
                both = []
                for p in range(2):
                    part = [r3[s, pl.ds(packed(i, whole, True, g, p, z + e), size_z, stride=pitch)]
                            for g in range(rows_k)]
                    guests = [None] * groups
                    for t, (h, g, shift) in enumerate(plan):
                        moved = pltpu.roll(part[first + h] * mask_ref[t], length - shift, axis=1)
                        guests[g] = moved if guests[g] is None else guests[g] + moved
                    for h in range(hosts):
                        part[first + h] = part[first + h] * mask_ref[len(plan) + h]
                    both += part + guests
                sides.append(jnp.concatenate(both, axis=0))
            done = left_dot(yi_ref, jnp.concatenate(sides, axis=1))
            for p in range(2):
                for e in range(2):
                    part = done[p * length : (p + 1) * length, e * length : (e + 1) * length]
                    r1[p, s, first_z + z + e] = part.reshape(size_y, rows_y, length)
        for d in order_y:
            copy4(i, whole, d).start()
        zs = pl.ds(first_z, n)
        o[:, me_y, s, zs] = r1[:, s, zs, me_y]

    def inverse_x(i, whole):
        s, z, n, _, _ = place(i, whole, True)
        zs = pl.ds(z, n)
        area = n * rows_y
        pot = pot_ref[zs].reshape(area, length)
        await_all(a1.at[:, pl.ds(0, size_y - 1), s, zs], q4.at[i])
        for d in range(size_y):
            owner = (me_y + size_y - d) % size_y
            rows = jnp.concatenate(
                [o[p, owner, s, zs].reshape(area, length) for p in range(2)], axis=1)
            done = right_dot(rows, xi_ref)
            fields, results = [], []
            for p in range(2):
                field = u[p, owner, s, zs].reshape(area, length)
                part = done[:, p * length : (p + 1) * length] + pot * field
                o[p, owner, s, zs] = part.reshape(n, rows_y, length)
                fields.append(field.reshape(area // 8, 8, length))
                results.append(part.reshape(area // 8, 8, length))

            def total(values):
                return jnp.sum(values[0] + values[1], axis=0)
            norm = total([f * f for f in fields])
            corr = total([f * r for f, r in zip(fields, results)])
            shift = jnp.where(norm > 0.0, corr / jnp.where(norm > 0.0, norm, 1.0), 0.0)
            gaps = [r - shift[None] * f for f, r in zip(fields, results)]
            values = (norm, corr, shift, total([g * g for g in gaps]),
                      total([g * f for g, f in zip(gaps, fields)]))
            for k, value in enumerate(values):
                sums[k, owner, s, z // step if whole else z // (step // 2) - (chunks - 1)] = value

    sums[:, :, :, chunks] = jnp.zeros((5, size_y, slots, 8, length), jnp.float32)
    fetches[1].wait()

    def before(i, carry):
        forward_x(i, False, False)
        return carry
    lax.fori_loop(0, 2, before, 0)
    pl.semaphore_wait(barrier, size_y + size_z - 2)
    for i in range(2):
        for d in order_y:
            copy1(i, False, d).start()
    for n, fetch in enumerate(fetches):
        if n != 1:
            fetch.wait()

    def outward(i, carry):
        @pl.when(i + 2 < units)
        def _():
            each(i + 2, forward_x, False)
        each(i, forward_y, False)

        @pl.when(i >= window)
        def _():
            each(i - window, arrive2, False)
        each(i, leave2, False)

        @pl.when(i == chunks + window)
        def _():
            both_z(0)
        return carry
    lax.fori_loop(0, units, outward, 0)

    def homeward(i, carry):
        @pl.when(i < window)
        def _():
            each(units - window + i, arrive2, False)

        @pl.when(i >= window)
        def _():
            each(i - window, arrive3, True)

        @pl.when(i < units)
        def _():
            each(i, leave3, True)

        @pl.when(i == window - 1)
        def _():
            both_z(1)

        @pl.when(i >= window)
        def _():
            each(i - window, inverse_y, True)

        @pl.when(i > window + 1)
        def _():
            each(i - window - 2, inverse_x, True)
        return carry
    lax.fori_loop(0, units + window, homeward, 0)
    for i in range(units - 2, units):
        inverse_x(i, False)

    norm, corr, shift, rest_sq, rest_dot = (
        sums[n].reshape(bands, (chunks + 1) * 8, length) for n in range(5))

    def of_band(value):
        return jnp.sum(jnp.sum(value, axis=1), axis=1, keepdims=True)
    norm_own, corr_own = of_band(norm), of_band(corr)
    shift_own = jnp.where(norm_own > 0.0, corr_own / jnp.where(norm_own > 0.0, norm_own, 1.0), 0.0)
    gap = shift - shift_own[:, :, None]
    sq_own = of_band(rest_sq + gap * (2.0 * rest_dot + gap * norm))
    dot_own = of_band(rest_dot + gap * norm)
    line = lax.broadcasted_iota(jnp.int32, (bands, length), 0)
    lane = lax.broadcasted_iota(jnp.int32, (bands, length), 1)
    packed = jnp.zeros((bands, length), jnp.float32)
    for n, value in enumerate((norm_own, corr_own, shift_own, sq_own, dot_own)):
        packed = jnp.where(lane == n * bands + line, value, packed)
    own[...] = jnp.sum(packed, axis=0, keepdims=True)
    me = me_y * size_z + me_z

    def tell(y, z):
        return pltpu.make_async_remote_copy(
            src_ref=own, dst_ref=every.at[me], send_sem=sg, recv_sem=qg,
            device_id={"py": (me_y + y) % size_y, "pz": (me_z + z) % size_z}, device_id_type=MESH)

    for z in order_z + [0]:
        for y in range(size_y):
            if y or z:
                tell(y, z).start()
    every[me] = own[...]
    free = jnp.zeros((1, length), jnp.float32)

    for n in range(bands):
        free = jnp.where(lane[:1] == n, 1.0 - locked_ref[n].astype(jnp.float32), free)
    every[count] = free
    for sem in (s1, s4):
        await_all(a1.at[:, pl.ds(0, size_y - 1)], sem)
    for s in range(slots):
        for sem, extra in ((s2, 8 * (s == 0)), (s3, 8 * (s == slots - 1))):
            await_all(a2.at[0, pl.ds(0, (size_z - 1) * (chunks * big + extra))], sem.at[s])
    for sem in (sg, qg):
        await_all(every.at[pl.ds(0, count - 1)], sem)


def finish_kernel(bands, applied_ref, every_ref, out_hbm, rayleigh_hbm, residual_hbm, ray, res, sems):
    copies = [pltpu.make_async_copy(src, dst, sems.at[n]) for n, (src, dst) in enumerate(
        ((applied_ref, out_hbm), (ray, rayleigh_hbm), (res, residual_hbm)))]
    copies[0].start()
    count, _, length = every_ref.shape
    count = count - 1
    table = every_ref[pl.ds(0, count)].reshape(count, length)
    total = jnp.broadcast_to(jnp.sum(table, axis=0, keepdims=True), (8, length))
    used = lax.broadcasted_iota(jnp.int32, (8, length), 1) < bands

    def kind(value, n):
        return pltpu.roll(value, length - n * bands, axis=1)
    norm_sq = jnp.where(used, total, 1.0)
    rayleigh = jnp.where(used, kind(total, 1), 0.0) / norm_sq
    gap = kind(table, 2) - rayleigh[:1]
    residual = kind(table, 3) + gap * (2.0 * kind(table, 4) + gap * table)
    residual = jnp.maximum(jnp.sum(residual, axis=0, keepdims=True), 0.0)
    residual = jnp.sqrt(jnp.where(used, residual, 0.0) / norm_sq)
    ray[...] = rayleigh[:1, :bands]
    res[...] = (residual[:1] * every_ref[count])[:, :bands]
    for copy in copies[1:]:
        copy.start()
    for copy in copies:
        copy.wait()


def two_parts(table):
    table = np.asarray(table, np.float64).astype(np.float32)
    high = table.astype(jnp.bfloat16)
    low = (table - high.astype(np.float32)).astype(jnp.bfloat16)
    return high, low


def exact_matrix(length, inverse):
    counter = np.arange(length)
    angle = 2.0 * math.pi / length * (counter[:, None] * counter[None, :] % length)
    if inverse:
        cosines, sines = np.cos(angle) / length, np.sin(angle) / length
    else:
        cosines, sines = np.cos(angle), -np.sin(angle)
    return np.block([[cosines, sines], [-sines, cosines]])


def fused_hamiltonian(wavefunctions, potential, cutoff_sq, locked_mask, folding, step):
    order, first, plan, masks, square = folding
    _, bands, rows_z, rows_y, length = wavefunctions.shape
    size_y, size_z = lax.axis_size("py"), lax.axis_size("pz")
    slots = bands // size_y
    rows_k = square.shape[0] // size_z
    chunks = rows_z // step
    units = slots * chunks + 1
    pitch = 2 * rows_z * rows_k + 8
    count = size_y * size_z
    xf, xi = exact_matrix(length, False), exact_matrix(length, True)
    both_y = np.concatenate([order, order + length])
    order_z = (rows_z * np.arange(size_z)[None, :] + np.arange(rows_z)[:, None]).reshape(-1)
    both_z = np.concatenate([order_z, order_z + length])
    tables = [np.concatenate(two_parts(t), axis=0) for t in (xf, xi)]
    tables += [np.concatenate(two_parts(t), axis=1)
               for t in (xf.T[:, both_z], xi.T[both_z], xf.T[both_y], xi.T[:, both_y])]
    tables = [jnp.asarray(t) for t in tables]
    squares = np.ascontiguousarray(square.reshape(rows_k, size_z, length).swapaxes(0, 1))
    xf_t, xi_t, lf_t, li_t, yf_t, yi_t = tables
    field = wavefunctions.reshape(2, size_y, slots, rows_z, rows_y, length)
    vmem = pl.BlockSpec(memory_space=pltpu.VMEM)
    anywhere = pl.BlockSpec(memory_space=pl.ANY)
    hbm = pl.BlockSpec(memory_space=pltpu.HBM)
    smem = pl.BlockSpec(memory_space=pltpu.SMEM)
    here = pltpu.SemaphoreType.DMA((units,))
    once = pltpu.SemaphoreType.DMA
    both = pltpu.SemaphoreType.DMA((slots,))
    f32 = jnp.float32
    in_hbm = functools.partial(pltpu.with_memory_space_constraint, memory_space=pltpu.HBM)
    in_vmem = functools.partial(pltpu.with_memory_space_constraint, memory_space=pltpu.VMEM)
    operands = (xf_t, yf_t, jnp.asarray(masks), lf_t, li_t, jnp.asarray(squares), yi_t, xi_t, potential)
    applied, every = pl.pallas_call(
        functools.partial(main_kernel, size_y, size_z, step, first, plan, WINDOW),
        out_shape=(pltpu.VMEM(field.shape, f32), pltpu.VMEM((count + 1, 1, length), f32)),
        in_specs=[hbm, smem] + [hbm] * (len(operands) + 1),
        out_specs=(vmem, vmem),
        scratch_shapes=[pltpu.VMEM(field.shape, f32), pltpu.SMEM((bands,), jnp.int32)]
        + [pltpu.VMEM(x.shape, x.dtype) for x in operands]
        + [
            pltpu.VMEM(field.shape, f32),
            pltpu.VMEM((2, slots, rows_z, size_y, rows_y, length), f32),
            pltpu.VMEM((slots, size_z * pitch, length), f32),
            pltpu.VMEM((slots, size_z * pitch, length), f32),
            pltpu.VMEM((slots, size_z * pitch, length), f32),
            pltpu.VMEM((slots, size_z * pitch, length), f32),
            pltpu.VMEM((5, size_y, slots, chunks + 1, 8, length), f32),
            pltpu.VMEM((1, length), f32),
            once, here, both, here, both, here, once, here, here,
            pltpu.SemaphoreType.DMA((len(operands) + 1,)), once, once,
        ],
        compiler_params=pltpu.CompilerParams(
            collective_id=0, has_side_effects=True, vmem_limit_bytes=48 * 1024 * 1024),
    )(in_hbm(field), cutoff_sq, *[in_hbm(x) for x in (locked_mask,) + operands])
    out, rayleigh, residual = pl.pallas_call(
        functools.partial(finish_kernel, bands),
        out_shape=(jax.ShapeDtypeStruct(field.shape, f32), jax.ShapeDtypeStruct((1, bands), f32),
                   jax.ShapeDtypeStruct((1, bands), f32)),
        in_specs=[anywhere, vmem],
        out_specs=(hbm, hbm, hbm),
        scratch_shapes=[pltpu.VMEM((1, bands), f32)] * 2 + [pltpu.SemaphoreType.DMA((3,))],
        compiler_params=pltpu.CompilerParams(vmem_limit_bytes=8 * 1024 * 1024),
    )(in_vmem(applied), in_vmem(every))
    return out.reshape(wavefunctions.shape), rayleigh.reshape(bands), residual.reshape(bands)


def gather_kernel(size_y, size_z, own_ref, out_ref, send, recv):
    me_y, me_z = lax.axis_index("py"), lax.axis_index("pz")
    me = me_y * size_z + me_z
    count = size_y * size_z
    barrier = pltpu.get_barrier_semaphore()

    def target(t):
        to = (me + t) % count
        return {"py": to // size_z, "pz": to % size_z}

    def greet(t, carry):
        pl.semaphore_signal(barrier, inc=1, device_id=target(t), device_id_type=MESH)
        return carry
    lax.fori_loop(1, count, greet, 0)
    pl.semaphore_wait(barrier, count - 1)

    def copy(t):
        return pltpu.make_async_remote_copy(
            src_ref=own_ref, dst_ref=out_ref.at[me], send_sem=send.at[t], recv_sem=recv.at[t],
            device_id=target(t), device_id_type=MESH)

    def leave(t, carry):
        copy(t).start()
        return carry
    lax.fori_loop(1, count, leave, 0)
    out_ref[me] = own_ref[...]

    def arrive(t, carry):
        copy(t).wait()
        return carry
    lax.fori_loop(1, count, arrive, 0)


def gather_sums(sums):
    size_y, size_z = lax.axis_size("py"), lax.axis_size("pz")
    count = size_y * size_z
    kinds, bands = sums.shape
    if count > 64:
        return lax.all_gather(sums, ("py", "pz"))
    own = jnp.pad(sums, ((0, 8 - kinds), (0, 128 - bands)))
    vmem = pl.BlockSpec(memory_space=pltpu.VMEM)
    every = pl.pallas_call(
        functools.partial(gather_kernel, size_y, size_z),
        out_shape=jax.ShapeDtypeStruct((count, 8, 128), jnp.float32),
        in_specs=[vmem],
        out_specs=vmem,
        scratch_shapes=[pltpu.SemaphoreType.DMA((count,)), pltpu.SemaphoreType.DMA((count,))],
        compiler_params=pltpu.CompilerParams(collective_id=1, has_side_effects=True),
    )(own)
    return every[:, :kinds, :bands]


def weigh(total, cutoff_sq, length):
    keep = (total <= cutoff_sq[0]).astype(jnp.float32)
    return 0.5 * (math.pi / length) ** 2 * total.astype(jnp.float32) * keep


def plain_kinetic(wavefunctions, kinetic, forward, inverse):
    along_x = "bzyn,kn->bzyk"
    along_y = "bznx,kn->bzkx"
    along_z = "bnyx,kn->bkyx"
    pair = (wavefunctions[0], wavefunctions[1])
    pair = transform(along_x, pair, forward)
    pair = exchange(pair, "py", 0, 2)
    pair = transform(along_y, pair, forward)
    pair = exchange(pair, "pz", 2, 1)
    pair = transform(along_z, pair, forward)
    pair = tuple(part * jnp.swapaxes(kinetic, 0, 1)[None] for part in pair)
    pair = transform(along_z, pair, inverse)
    pair = exchange(pair, "pz", 1, 2)
    pair = transform(along_y, pair, inverse)
    pair = exchange(pair, "py", 2, 0)
    pair = transform(along_x, pair, inverse)
    return jnp.stack(pair)


def body(wavefunctions, potential, cutoff_sq, locked_mask):
    _, bands, rows_z, rows_y, length = wavefunctions.shape
    size_y, size_z = lax.axis_size("py"), lax.axis_size("pz")
    step = 4
    unlocked = 1.0 - locked_mask.astype(jnp.float32)
    fits = size_z == 8 and bands == 8 and length % 128 == 0
    fits = fits and rows_z % step == 0 and rows_z > step and rows_y % 8 == 0
    fits = fits and bands == 2 * size_y
    folding = None
    if fits:
        folding = fold_rows(length, size_z, 3 * size_z) or fold_rows(length, size_z, 2 * size_z)
    if folding is not None:
        return fused_hamiltonian(
            wavefunctions, potential, cutoff_sq, locked_mask, folding, step)
    forward = make_tables(length, False)
    inverse = make_tables(length, True)
    rows = length // size_z
    full_sq = signed_square(jnp.arange(length, dtype=jnp.int32), length)
    own = lax.axis_index("pz") * rows + jnp.arange(rows, dtype=jnp.int32)
    own_sq = signed_square(own, length)
    total = own_sq[:, None, None] + full_sq[None, :, None] + full_sq[None, None, :]
    kinetic = weigh(total, cutoff_sq, length)
    back = plain_kinetic(wavefunctions, kinetic, forward, inverse)
    applied = back + potential[None, None] * wavefunctions
    norm_own = jnp.sum(wavefunctions * wavefunctions, axis=(0, 2, 3, 4))
    corr_own = jnp.sum(wavefunctions * applied, axis=(0, 2, 3, 4))
    shift = jnp.where(norm_own > 0.0, corr_own / jnp.where(norm_own > 0.0, norm_own, 1.0), 0.0)
    rest = applied - shift[None, :, None, None, None] * wavefunctions
    rest_sq = jnp.sum(rest * rest, axis=(0, 2, 3, 4))
    rest_dot = jnp.sum(rest * wavefunctions, axis=(0, 2, 3, 4))
    sums = jnp.stack([norm_own, corr_own, shift, rest_sq, rest_dot])
    every = gather_sums(sums)
    norm_all, corr_all, shift_all, sq_all, dot_all = (every[:, i] for i in range(5))
    norm_sq = jnp.sum(norm_all, axis=0)
    rayleigh = jnp.sum(corr_all, axis=0) / norm_sq
    gap = shift_all - rayleigh[None]
    residual_sq = jnp.sum(sq_all + 2.0 * gap * dot_all + gap * gap * norm_all, axis=0)
    residual_sq = jnp.maximum(residual_sq, 0.0)
    residual_norm = jnp.sqrt(residual_sq / norm_sq) * unlocked
    return (applied, rayleigh, residual_norm)


def solution(mesh):
    in_specs = (P(None, None, "pz", "py", None), P("pz", "py", None), P(), P())
    out_specs = (P(None, None, "pz", "py", None), P(), P())
    return jax.shard_map(body, mesh=mesh, in_specs=in_specs, out_specs=out_specs, check_vma=False)
```
